512 devices in a mesh: ens: 4 (over y), lat: 16 (over z), lon: 8 (over x, core).
Axes of the slice: x: 4, y: 4, z: 16, core: 2. Of those that a mesh axis runs over, the one named last changes fastest.
Arguments:
- maxima: float32 [128, 512, 4096], P('ens', 'lat', 'lon'), may hold values from 15 to 150
- latent: float32 [3, 512, 4096], P(None, 'lat', 'lon'), may hold values from 1 to 3, as said below
- coupling: float32 [3, 3], replicated, may hold values from -7.2 to 32, as said below
- local_precision: float32 [3, 512, 4096], P(None, 'lat', 'lon'), may hold values from 0.64 to 192, as said below
Outputs:
- solution: float32 [3, 512, 4096], P(None, 'lat', 'lon')
The draws below stay inside these ranges and needn't reach their ends.
Inputs may be any that keep to these rules, and one draw needn't show every extreme that they name: latent[0] lies in 1 to 2.5, latent[1] in log 10 to log 20, latent[2] in 1 to 2.5. coupling is symmetric with a dominant positive diagonal. `local_precision`: positive.
All inputs are finite; a program needn't handle non-finite values.
Results may differ from the reference program's by a relative error of at most 0.0001.
Values sent between devices are 32-bit elements; how exact they have to be, the bound alone decides.
No kernel may reach another device: no remote copies, remote signals or barrier semaphores. Data moves between devices by JAX's collectives and lax.ppermute only.
A program may use at most 64 MiB of HBM per device.

```python
import math
import jax
import jax.numpy as jnp
from jax import lax

MAX_DEV = 32
ITERS = 3
MAXIMA = 128
NLAT = 512
NLON = 4096
N_ENS = 4


def draw_latent(key, part):
    uniform_draw = jax.random.uniform(key, (3, NLAT, NLON), jnp.float32)
    lower_end = jnp.array([1.0, math.log(10.0), 1.0], jnp.float32)
    upper_end = jnp.array([2.5, math.log(20.0), 2.5], jnp.float32)
    return lower_end[:, None, None] + (upper_end - lower_end)[:, None, None] * uniform_draw


def draw_coupling(key, part):
    key_diag = jax.random.fold_in(key, 11)
    key_size = jax.random.fold_in(key, 12)
    key_sign = jax.random.fold_in(key, 13)
    diagonal = jax.random.uniform(key_diag, (3,), jnp.float32, 1.0, 2.0)
    magnitude = jax.random.uniform(key_size, (3, 3), jnp.float32, 0.25, 0.45)
    sign_draw = jnp.where(jax.random.bernoulli(key_sign, 0.5, (3, 3)), 1.0, -1.0)
    upper_part = jnp.triu(magnitude * sign_draw, 1)
    off_diagonal = upper_part + upper_part.T
    return (off_diagonal + jnp.diag(diagonal)) * (MAXIMA / 8.0)


def draw_local_precision(key, part):
    key_level = jax.random.fold_in(key, 21)
    uniform_draw = jax.random.uniform(key_level, (3, NLAT, NLON), jnp.float32)
    factors = jnp.array([3.0, 1.0, 1.0 / 3.0], jnp.float32)
    log_low = math.log(0.02)
    log_high = math.log(0.5)
    base = jnp.exp(log_low + (log_high - log_low) * uniform_draw)
    return base * factors[:, None, None] * MAXIMA


def levels(rng, shape, shards, low, top_value):
    factor_of, own = 1.0, jax.random.fold_in(rng, 6)
    for dim, parts in shards:
        steps = jnp.exp(jax.random.uniform(jax.random.fold_in(own, dim), (parts,), jnp.float32, low / len(shards), top_value / len(shards)))
        factor_of = factor_of * jnp.repeat(steps, shape[dim] // parts).reshape([-1 if axis == dim else 1 for axis in range(len(shape))])
    return factor_of


def setup_inputs(seed: int = 0) -> dict:
    keys = jax.random.split(jax.random.key(seed), 5)
    return {
        "maxima": jnp.clip(jnp.exp(math.log(150.0) - 2.3025851 * jax.random.uniform(keys[0], (MAXIMA, NLAT, NLON), jnp.float32) ** levels(keys[0], (MAXIMA, NLAT, NLON), ((0, 4), (1, 16), (2, 8)), -0.2, 0.2)), 15.0, 150.0),
        "latent": draw_latent(jax.random.fold_in(keys[4], 71), 0),
        "coupling": draw_coupling(jax.random.fold_in(keys[4], 71), 0),
        "local_precision": draw_local_precision(jax.random.fold_in(keys[4], 71), 0),
    }


def gev_terms(maxima, latent):
    loc_par = 10.0 * latent[0]
    scale_par = jnp.exp(latent[1])
    shape_par = 0.1 * latent[2]
    scaled = (maxima - loc_par) / scale_par
    inside = 1.0 + shape_par * scaled
    log_inside = jnp.log(inside)
    tail_term = jnp.exp(-log_inside / shape_par)
    common_term = (1.0 + shape_par - tail_term) / inside
    score_loc = 10.0 * common_term / scale_par
    score_scale = scaled * common_term - 1.0
    score_shape = 0.1 * (log_inside * (1.0 - tail_term) / (shape_par * shape_par) - scaled * common_term / shape_par)
    scores = jnp.stack([jnp.sum(score_loc, 0), jnp.sum(score_scale, 0), jnp.sum(score_shape, 0)])
    hessian = jnp.stack([
        jnp.sum(score_loc * score_loc, 0), jnp.sum(score_loc * score_scale, 0), jnp.sum(score_loc * score_shape, 0),
        jnp.sum(score_scale * score_scale, 0), jnp.sum(score_scale * score_shape, 0), jnp.sum(score_shape * score_shape, 0)])
    return scores, hessian


def mix_rows(coupling, laplace_term):
    return jnp.stack([
        coupling[0, 0] * laplace_term[0] + coupling[0, 1] * laplace_term[1] + coupling[0, 2] * laplace_term[2],
        coupling[1, 0] * laplace_term[0] + coupling[1, 1] * laplace_term[1] + coupling[1, 2] * laplace_term[2],
        coupling[2, 0] * laplace_term[0] + coupling[2, 1] * laplace_term[1] + coupling[2, 2] * laplace_term[2]])


def prior_apply(vector, coupling, local_precision):
    padded = jnp.pad(vector, ((0, 0), (1, 1), (1, 1)))
    beside = padded[:, 2:, 1:-1] + padded[:, :-2, 1:-1] + padded[:, 1:-1, 2:] + padded[:, 1:-1, :-2]
    laplace_term = 4.0 * vector - beside
    return mix_rows(coupling, laplace_term) + local_precision * vector


def hessian_apply(vector, hessian):
    return jnp.stack([
        hessian[0] * vector[0] + hessian[1] * vector[1] + hessian[2] * vector[2],
        hessian[1] * vector[0] + hessian[3] * vector[1] + hessian[4] * vector[2],
        hessian[2] * vector[0] + hessian[4] * vector[1] + hessian[5] * vector[2]])


def reference(maxima, latent, coupling, local_precision):
    blocks = maxima.reshape(N_ENS, MAX_DEV, NLAT, NLON)

    def add_block(carry, block):
        scores_part, hessian_part = gev_terms(block, latent)
        return (carry[0] + scores_part, carry[1] + hessian_part), None

    start = (jnp.zeros((3, NLAT, NLON), jnp.float32), jnp.zeros((6, NLAT, NLON), jnp.float32))
    (scores, hessian), unused = lax.scan(add_block, start, blocks)
    solution = latent
    residual = scores - prior_apply(latent, coupling, local_precision)
    direction = residual
    norm_now = jnp.sum(residual * residual)
    for iteration in range(ITERS):
        image = prior_apply(direction, coupling, local_precision) + hessian_apply(direction, hessian)
        step_size = norm_now / jnp.sum(direction * image)
        solution = solution + step_size * direction
        residual = residual - step_size * image
        norm_next = jnp.sum(residual * residual)
        direction = residual + (norm_next / norm_now) * direction
        norm_now = norm_next
    return solution
```

```python
import jax
import jax.numpy as jnp
from jax import lax
from jax.sharding import Mesh
from jax.sharding import PartitionSpec as P

ITERS = 3
LON = ("lon_0", "lon_1")
SCALE = 2.0**-10


def with_halo(value, sides, width):
    edges = {}
    for axis, dim in sides:
        devices, length = (lax.axis_size(axis), value.shape[dim])
        up = [(i, (i + 1) % devices) for i in range(devices - 1)]
        last = lax.slice_in_dim(value, length - width, length, axis=dim)
        first = lax.slice_in_dim(value, 0, width, axis=dim)
        edges[dim] = (
            lax.ppermute(last, axis, up),
            lax.ppermute(first, axis, [(b, a) for a, b in up]),
        )
    done = []
    for _, dim in sides:
        low, high = edges[dim]
        around = [(width, width) if d in done else (0, 0) for d in range(value.ndim)]
        value = jnp.concatenate([jnp.pad(low, around), value, jnp.pad(high, around)], axis=dim)
        done.append(dim)
    return value


def sent_to_all(value, axis):
    copies = jnp.broadcast_to(value, (lax.axis_size(axis), *value.shape))
    return lax.all_to_all(copies, axis, split_axis=0, concat_axis=0, tiled=True)


def over_copies(value, axis):
    return sent_to_all(value, axis).sum(axis=0)


def together(arrays, axis):
    ends = [0]
    for a in arrays:
        ends.append(ends[-1] + a.size)
    so_far = over_copies(jnp.concatenate([a.ravel() for a in arrays]), axis)
    return tuple((so_far[b:e].reshape(a.shape) for a, b, e in zip(arrays, ends, ends[1:])))


def moments_total(products):
    packed = jnp.stack([jnp.sum(p) for p in products])[None]
    return over_copies(over_copies(packed, LON), "lat")[0]


def krylov_weights(m):
    def inner(p, q, shift):
        return sum(p[i] * q[j] * m[i + j + shift] for i in range(len(p)) for j in range(len(q)))

    def combine(p, factor, q):
        n = max(len(p), len(q))
        p, q = (list(c) + [jnp.zeros((), m.dtype)] * (n - len(c)) for c in (p, q))
        return [x + factor * y for x, y in zip(p, q)]

    one, zero = jnp.ones((), m.dtype), jnp.zeros((), m.dtype)
    weights, residual, direction = [zero], [one], [one]
    norm_now = m[0]
    for iteration in range(ITERS):
        step_size = norm_now / inner(direction, direction, 1)
        weights = combine(weights, step_size, direction)
        if iteration + 1 < ITERS:
            residual = combine(residual, -step_size, [zero] + direction)
            norm_next = inner(residual, residual, 0)
            direction = combine(residual, norm_next / norm_now, direction)
            norm_now = norm_next
    return [SCALE * w for w in weights]


def gev_terms(maxima, latent):
    loc_par = 10.0 * latent[0]
    scale_par = jnp.exp(latent[1])
    shape_par = 0.1 * latent[2]
    scaled = (maxima - loc_par) / scale_par
    inside = 1.0 + shape_par * scaled
    log_inside = jnp.log(inside)
    tail_term = jnp.exp(-log_inside / shape_par)
    common_term = (1.0 + shape_par - tail_term) / inside
    score_loc = 10.0 * common_term / scale_par
    score_scale = scaled * common_term - 1.0
    score_shape = 0.1 * (
        log_inside * (1.0 - tail_term) / (shape_par * shape_par) - scaled * common_term / shape_par
    )
    scores = jnp.stack([jnp.sum(score_loc, 0), jnp.sum(score_scale, 0), jnp.sum(score_shape, 0)])
    hessian = jnp.stack(
        [
            jnp.sum(score_loc * score_loc, 0),
            jnp.sum(score_loc * score_scale, 0),
            jnp.sum(score_loc * score_shape, 0),
            jnp.sum(score_scale * score_scale, 0),
            jnp.sum(score_scale * score_shape, 0),
            jnp.sum(score_shape * score_shape, 0),
        ]
    )
    return (scores, hessian)


def mix_rows(coupling, laplace_term):
    return jnp.stack(
        [
            coupling[0, 0] * laplace_term[0]
            + coupling[0, 1] * laplace_term[1]
            + coupling[0, 2] * laplace_term[2],
            coupling[1, 0] * laplace_term[0]
            + coupling[1, 1] * laplace_term[1]
            + coupling[1, 2] * laplace_term[2],
            coupling[2, 0] * laplace_term[0]
            + coupling[2, 1] * laplace_term[1]
            + coupling[2, 2] * laplace_term[2],
        ]
    )


def tile_pad(vector):
    return with_halo(vector, (("lat", 1), (LON, 2)), 1)


def prior_apply(vector, coupling, local_precision, padder):
    padded = padder(vector)
    beside = padded[:, 2:, 1:-1] + padded[:, :-2, 1:-1] + padded[:, 1:-1, 2:] + padded[:, 1:-1, :-2]
    laplace_term = 4.0 * vector - beside
    return mix_rows(coupling, laplace_term) + local_precision * vector


def hessian_apply(vector, hessian):
    return jnp.stack(
        [
            hessian[0] * vector[0] + hessian[1] * vector[1] + hessian[2] * vector[2],
            hessian[1] * vector[0] + hessian[3] * vector[1] + hessian[4] * vector[2],
            hessian[2] * vector[0] + hessian[4] * vector[1] + hessian[5] * vector[2],
        ]
    )


def per_device(maxima, latent, coupling, local_precision):
    scores_local, hessian_local = gev_terms(maxima, latent)
    scores, hessian = together((scores_local, hessian_local), "ens")

    def operate(vector):
        return SCALE * (
            prior_apply(vector, coupling, local_precision, tile_pad)
            + hessian_apply(vector, hessian)
        )

    basis = [scores - prior_apply(latent, coupling, local_precision, tile_pad)]
    for _ in range(ITERS):
        basis.append(operate(basis[-1]))
    products = [basis[k // 2] * basis[k - k // 2] for k in range(2 * ITERS)]
    weights = krylov_weights(moments_total(products))
    return latent + weights[0] * basis[0] + weights[1] * basis[1] + weights[2] * basis[2]


def solution(mesh):
    split = Mesh(
        mesh.devices.reshape(mesh.shape["ens"], mesh.shape["lat"], 4, 2),
        ("ens", "lat", "lon_0", "lon_1"),
    )
    placed = (P("ens", "lat", LON), P(None, "lat", LON), P(), P(None, "lat", LON))
    return jax.shard_map(
        per_device, mesh=split, in_specs=placed, out_specs=P(None, "lat", LON), check_vma=False
    )
```

```python
import itertools

import jax
import jax.numpy as jnp
from jax import lax
from jax.experimental import pallas as pl
from jax.experimental.pallas import tpu as pltpu
from jax.sharding import Mesh
from jax.sharding import PartitionSpec as P

ITERS = 3
LON = ("lon_0", "lon_1")
EVERY = ("ens", "lat", *LON)
SCALE = 2.0**-10
INTERPRET = False

ROWS, COLS = 32, 512
SUMS = 9
FIELDS = 12
HALO = 4
EDGE_AT = SUMS * 2 * 16
SIDE_AT = EDGE_AT + SUMS * 2 * HALO
PART_ROWS = SIDE_AT + 24

VMEM = pl.BlockSpec(memory_space=pltpu.VMEM)
SMEM = pl.BlockSpec(memory_space=pltpu.SMEM)


def lanes_of(field, shape):
    lane = lax.broadcasted_iota(jnp.int32, shape, 1)
    return (lane >= HALO * field) & (lane < HALO * (field + 1))


def pack_sides(columns, first):
    packed = jnp.zeros(columns[0].shape, jnp.float32)
    for f, x in enumerate(columns):
        shift = (HALO * f if first else HALO * f + HALO - 128) % 128
        packed = jnp.where(lanes_of(f, x.shape), pltpu.roll(x, shift, 1) if shift else x, packed)
    return packed


def unpack_side(packed, field, first):
    shift = (-HALO * field if first else 128 - HALO - HALO * field) % 128
    return pltpu.roll(packed, shift, 1) if shift else packed


def gev_kernel(maxima_ref, latent_ref, part_ref):
    block = pl.program_id(0)
    for half in range(2):
        cols = slice(256 * half, 256 * half + 256)
        loc_par = 10.0 * latent_ref[0, :, cols]
        per_scale = jnp.exp(-latent_ref[1, :, cols])
        shape_par = 0.1 * latent_ref[2, :, cols]
        per_shape = 1.0 / shape_par

        def add_one(m, sums):
            scaled = (maxima_ref[m, :, cols] - loc_par) * per_scale
            inside = 1.0 + shape_par * scaled
            exponent = jnp.log(inside) * per_shape
            rest = 1.0 - jnp.exp(-exponent)
            a = (shape_par + rest) / inside
            sa = scaled * a
            b = sa - 1.0
            c = exponent * rest - sa
            terms = (a, b, c, a * a, a * b, a * c, b * b, b * c, c * c)
            return tuple(s + t for s, t in zip(sums, terms))

        zero = jnp.zeros((8, 256), jnp.float32)
        sums = lax.fori_loop(0, maxima_ref.shape[0], add_one, (zero,) * SUMS, unroll=4)
        ka, kc = 10.0 * per_scale, 0.1 * per_shape
        factors = (ka, None, kc, ka * ka, ka, ka * kc, None, kc, kc * kc)
        sums = [s if k is None else s * k for s, k in zip(sums, factors)]

        owner = 2 * (block // 2) + half
        for f in range(SUMS):
            for t in range(2):
                at = pl.multiple_of((2 * f + t) * 16 + 8 * (block % 2), 8)
                part_ref[owner, pl.ds(at, 8), :] = sums[f][:, 128 * t : 128 * t + 128]

        def put_edge(to, rows):
            for f in range(SUMS):
                for t in range(2):
                    at = EDGE_AT + (2 * f + t) * HALO
                    part_ref[to, at : at + HALO, :] = sums[f][rows, 128 * t : 128 * t + 128]

        pl.when(block == 2)(lambda: put_edge(half, slice(0, HALO)))
        pl.when(block == 1)(lambda: put_edge(2 + half, slice(8 - HALO, 8)))

        near = slice(0, 128) if half else slice(128, 256)
        side = pack_sides([s[:, near] for s in sums], bool(half))

        def put_side(to, tile):
            part_ref[to, pl.ds(pl.multiple_of(SIDE_AT + 8 * tile, 8), 8), :] = side

        pl.when(block <= 2)(lambda: put_side(1 - half, block))
        pl.when(block >= 1)(lambda: put_side(3 - half, block - 1))


def placing(er, ec):
    return dict(
        rows=slice(8, 32) if er == 0 else slice(0, 24),
        cols=slice(128, 512) if ec == 0 else slice(0, 384),
        tile_rows=slice(0, 24) if er == 0 else slice(8, 32),
        tile_cols=slice(0, 384) if ec == 0 else slice(128, 512),
        inner_rows=slice(24, 28) if er == 0 else slice(4, 8),
        outer_rows=slice(4, 8) if er == 0 else slice(24, 28),
        own_edge=slice(8, 12) if er == 0 else slice(20, 24),
        tile_edge=slice(0, 4) if er == 0 else slice(28, 32),
        inner_cols=slice(384, 512) if ec == 0 else slice(0, 128),
        outer_cols=slice(0, 128) if ec == 0 else slice(384, 512),
        own_side=slice(128, 256) if ec == 0 else slice(256, 384),
        tile_side=slice(0, 128) if ec == 0 else slice(384, 512),
        corner=slice(0, 8) if er == 0 else slice(16, 24),
    )


def for_quarter(body):
    mine = lax.axis_index("ens")
    for e in range(4):
        pl.when(mine == e)(lambda e=e: body(e // 2, e % 2, placing(e // 2, e % 2)))


def join_kernel(got_ref, latent_ref, precision_ref, window_ref, edge_ref, side_ref, corner_ref):
    def body(er, ec, at):
        def total(start, rows):
            cut = slice(start, start + rows)
            return got_ref[0, cut, :] + got_ref[1, cut, :] + got_ref[2, cut, :] + got_ref[3, cut, :]

        window_ref[...] = jnp.zeros(window_ref.shape, jnp.float32)
        sides = total(SIDE_AT, 24)
        for f in range(SUMS):
            window_ref[f, at["rows"], at["inner_cols"]] = unpack_side(sides, f, ec == 0)
            for t in range(2):
                cols = slice(128 + 128 * t, 256 + 128 * t)
                window_ref[f, 8:24, cols] = total((2 * f + t) * 16, 16)
                window_ref[f, at["inner_rows"], cols] = total(EDGE_AT + (2 * f + t) * HALO, HALO)
        for k, diagonal in enumerate((3, 6, 8)):
            level = precision_ref[k, at["tile_rows"], at["tile_cols"]]
            here = latent_ref[k, at["tile_rows"], at["tile_cols"]]
            there = (at["rows"], at["cols"])
            window_ref[k, *there] = window_ref[k, *there] - level * here
            window_ref[diagonal, *there] = window_ref[diagonal, *there] + level
        for f in range(FIELDS):
            edge_ref[HALO * f : HALO * f + HALO, :] = (
                window_ref[f, at["own_edge"], at["cols"]]
                if f < SUMS
                else latent_ref[f - SUMS, at["tile_edge"], at["tile_cols"]]
            )
        columns = [window_ref[f, at["rows"], at["own_side"]] for f in range(SUMS)]
        columns += [latent_ref[k, at["tile_rows"], at["tile_side"]] for k in range(3)]
        side = pack_sides(columns, ec == 0)
        side_ref[...] = side
        corner_ref[...] = side[at["corner"], :]

    for_quarter(body)


def krylov_kernel(
    coupling_ref, window_ref, latent_ref, edge_ref, side_ref, corner_ref, basis_ref, moments_ref, full_ref
):
    def body(er, ec, at):
        full_ref[0:SUMS] = window_ref[...]
        full_ref[SUMS:FIELDS, at["rows"], at["cols"]] = latent_ref[:, at["tile_rows"], at["tile_cols"]]
        parts = [corner_ref[...], side_ref[...]] if er == 0 else [side_ref[...], corner_ref[...]]
        sides = jnp.concatenate(parts, axis=0)
        for f in range(FIELDS):
            full_ref[f, at["outer_rows"], at["cols"]] = edge_ref[HALO * f : HALO * f + HALO, :]
            full_ref[f, :, at["outer_cols"]] = unpack_side(sides, f, ec == 1)

    for_quarter(body)
    mine = lax.axis_index("ens")
    lon = lax.axis_index(LON[0]) * lax.axis_size(LON[1]) + lax.axis_index(LON[1])
    n_lon = lax.axis_size(LON[0]) * lax.axis_size(LON[1])
    shape = (ROWS, COLS)
    row = lax.broadcasted_iota(jnp.int32, shape, 0) + (
        lax.axis_index("lat") * ROWS + 16 * (mine // 2) - 8
    )
    col = lax.broadcasted_iota(jnp.int32, shape, 1) + (lon * COLS + 256 * (mine % 2) - 128)
    inside = (row >= 0) & (row < lax.axis_size("lat") * ROWS) & (col >= 0) & (col < n_lon * COLS)

    def mixed(field):
        laplace = []
        for x in field:
            beside = pltpu.roll(x, 1, 0) + pltpu.roll(x, ROWS - 1, 0)
            beside = beside + (pltpu.roll(x, 1, 1) + pltpu.roll(x, COLS - 1, 1))
            laplace.append(4.0 * x - beside)
        return [
            coupling_ref[k, 0] * laplace[0]
            + coupling_ref[k, 1] * laplace[1]
            + coupling_ref[k, 2] * laplace[2]
            for k in range(3)
        ]

    def operate(field):
        q = mixed(field)
        h = [full_ref[3 + k] for k in range(6)]
        x, y, z = field
        own = (h[0] * x + h[1] * y + h[2] * z, h[1] * x + h[3] * y + h[4] * z, h[2] * x + h[4] * y + h[5] * z)
        return [jnp.where(inside, SCALE * (a + b), 0.0) for a, b in zip(q, own)]

    prior = mixed([full_ref[SUMS + k] for k in range(3)])
    basis = [[jnp.where(inside, full_ref[k] - prior[k], 0.0) for k in range(3)]]
    for _ in range(ITERS):
        basis.append(operate(basis[-1]))
    own = [[x[8:24, 128:384] for x in field] for field in basis]
    for p in range(ITERS):
        for k in range(3):
            basis_ref[3 * p + k] = own[p][k]
    rows = []
    for k in range(2 * ITERS):
        a, b = own[k // 2], own[k - k // 2]
        product = a[0] * b[0] + a[1] * b[1] + a[2] * b[2]
        product = product[:, :128] + product[:, 128:]
        rows.append(jnp.sum(product, axis=0, keepdims=True))
    rows.append(jnp.zeros((2, 128), jnp.float32))
    moments_ref[...] = jnp.broadcast_to(jnp.concatenate(rows, axis=0)[None], moments_ref.shape)


def krylov_weights(m):
    def inner(p, q, shift):
        terms = [p[i] * q[j] * m[i + j + shift] for i in range(len(p)) for j in range(len(q))]
        return sum(terms[1:], terms[0])

    def combine(p, factor, q):
        both = [x + factor * y for x, y in zip(p, q)]
        return both + p[len(q) :] + [factor * y for y in q[len(p) :]]

    one = jnp.ones_like(m[0])
    zero = jnp.zeros_like(m[0])
    weights, residual, direction = [], [one], [one]
    norm_now = m[0]
    for iteration in range(ITERS):
        step_size = norm_now / inner(direction, direction, 1)
        weights = combine(weights, step_size, direction)
        if iteration + 1 < ITERS:
            residual = combine(residual, -step_size, [zero] + direction)
            norm_next = inner(residual, residual, 0)
            direction = combine(residual, norm_next / norm_now, direction)
            norm_now = norm_next
    return [SCALE * w for w in weights]


def update_kernel(moments_ref, latent_ref, *refs):
    basis_refs, solution_ref = refs[:-1], refs[-1]
    moments = jnp.sum(jnp.sum(moments_ref[...], axis=0), axis=1, keepdims=True)
    weights = krylov_weights([moments[k : k + 1, :] for k in range(2 * ITERS)])
    weights = [jnp.broadcast_to(w, (16, 256)) for w in weights]
    mine = lax.axis_index("ens")
    for back, basis_ref in enumerate(basis_refs):
        e = lax.rem(mine + (4 - back), 4)
        rows = pl.ds(pl.multiple_of(16 * (e // 2), 8), 16)
        cols = pl.ds(pl.multiple_of(256 * (e % 2), 128), 256)
        for k in range(3):
            step = weights[0] * basis_ref[k] + weights[1] * basis_ref[3 + k] + weights[2] * basis_ref[6 + k]
            solution_ref[k, rows, cols] = latent_ref[k, rows, cols] + step


def f32(*shape):
    return jax.ShapeDtypeStruct(shape, jnp.float32)


def to_neighbour(value, where):
    sizes = [lax.axis_size(axis) for axis in EVERY]
    n_lat, n_lon = sizes[1], sizes[2] * sizes[3]
    pairs = []
    for e, lat, lon in itertools.product(range(4), range(n_lat), range(n_lon)):
        e_to, lat_to, lon_to = where(e, lat, lon)
        if 0 <= lat_to < n_lat and 0 <= lon_to < n_lon:
            pairs.append(((e * n_lat + lat) * n_lon + lon, (e_to * n_lat + lat_to) * n_lon + lon_to))
    return lax.ppermute(value, EVERY, pairs)


def step_of(side):
    return 1 if side else -1


def per_device(maxima, latent, coupling, local_precision):
    depth = maxima.shape[0]
    part = pl.pallas_call(
        gev_kernel,
        grid=(4,),
        in_specs=[
            pl.BlockSpec((depth, 8, COLS), lambda i: (0, i, 0)),
            pl.BlockSpec((3, 8, COLS), lambda i: (0, i, 0)),
        ],
        out_specs=VMEM,
        out_shape=f32(4, PART_ROWS, 128),
        interpret=INTERPRET,
        name="gev",
    )(maxima, latent)
    got = lax.all_to_all(part, "ens", 0, 0, tiled=True)
    window, edge, side, corner = pl.pallas_call(
        join_kernel,
        in_specs=[VMEM] * 3,
        out_specs=[VMEM] * 4,
        out_shape=[f32(SUMS, ROWS, COLS), f32(FIELDS * HALO, 384), f32(24, 128), f32(8, 128)],
        interpret=INTERPRET,
        name="join",
    )(got, latent, local_precision)
    edge = to_neighbour(edge, lambda e, lat, lon: (e ^ 2, lat + step_of(e // 2), lon))
    side = to_neighbour(side, lambda e, lat, lon: (e ^ 1, lat, lon + step_of(e % 2)))
    corner = to_neighbour(corner, lambda e, lat, lon: (e ^ 3, lat + step_of(e // 2), lon + step_of(e % 2)))
    n_lat = lax.axis_size("lat")
    basis, moments = pl.pallas_call(
        krylov_kernel,
        in_specs=[SMEM] + [VMEM] * 5,
        out_specs=[VMEM] * 2,
        out_shape=[f32(3 * ITERS, 16, 256), f32(n_lat, 8, 128)],
        scratch_shapes=[pltpu.VMEM((FIELDS, ROWS, COLS), jnp.float32)],
        interpret=INTERPRET,
        name="krylov",
    )(coupling, window, latent, edge, side, corner)
    others = [lax.ppermute(basis, "ens", [(e, (e + k) % 4) for e in range(4)]) for k in range(1, 4)]
    moments = lax.all_to_all(moments, "lat", 0, 0, tiled=True).sum(axis=0)
    rest = ("ens", *LON)
    moments = jnp.broadcast_to(moments, (lax.axis_size(rest), *moments.shape))
    moments = lax.all_to_all(moments, rest, 0, 0, tiled=True)
    return pl.pallas_call(
        update_kernel,
        in_specs=[VMEM] * 6,
        out_specs=VMEM,
        out_shape=f32(3, ROWS, COLS),
        interpret=INTERPRET,
        name="update",
    )(moments, latent, basis, *others)


def solution(mesh):
    split = Mesh(
        mesh.devices.reshape(mesh.shape["ens"], mesh.shape["lat"], -1, 2),
        ("ens", "lat", "lon_0", "lon_1"),
    )
    placed = (P("ens", "lat", LON), P(None, "lat", LON), P(), P(None, "lat", LON))
    return jax.shard_map(
        per_device, mesh=split, in_specs=placed, out_specs=P(None, "lat", LON), check_vma=False
    )
```

```python
import itertools

import jax
import jax.numpy as jnp
from jax import lax
from jax.experimental import pallas as pl
from jax.experimental.pallas import tpu as pltpu
from jax.sharding import Mesh
from jax.sharding import PartitionSpec as P

ITERS = 3
LON = ("lon_0", "lon_1")
EVERY = ("ens", "lat", *LON)
SCALE = 2.0**-10
INTERPRET = False

ROWS, COLS = 32, 512
SUMS = 9
FIELDS = 12
HALO = 4
EDGE_AT = SUMS * 2 * 16
SIDE_AT = EDGE_AT + SUMS * 2 * HALO
PART_ROWS = SIDE_AT + 24

VMEM = pl.BlockSpec(memory_space=pltpu.VMEM)
SMEM = pl.BlockSpec(memory_space=pltpu.SMEM)


def lanes_of(field, shape):
    lane = lax.broadcasted_iota(jnp.int32, shape, 1)
    return (lane >= HALO * field) & (lane < HALO * (field + 1))


def pack_sides(columns, first):
    packed = jnp.zeros(columns[0].shape, jnp.float32)
    for f, x in enumerate(columns):
        shift = (HALO * f if first else HALO * f + HALO - 128) % 128
        packed = jnp.where(lanes_of(f, x.shape), pltpu.roll(x, shift, 1) if shift else x, packed)
    return packed


def unpack_side(packed, field, first):
    shift = (-HALO * field if first else 128 - HALO - HALO * field) % 128
    return pltpu.roll(packed, shift, 1) if shift else packed


def place_of_lon():
    return lax.axis_index(LON[0]) * lax.axis_size(LON[1]) + lax.axis_index(LON[1])


def swapped(e):
    return 2 * ((e // 2 + lax.axis_index("lat")) % 2) + (e + place_of_lon()) % 2


def gev_kernel(maxima_ref, latent_ref, part_ref):
    block = pl.program_id(0)
    for half in range(2):
        cols = slice(256 * half, 256 * half + 256)
        loc_par = 10.0 * latent_ref[0, :, cols]
        per_scale = jnp.exp(-latent_ref[1, :, cols])
        shape_par = 0.1 * latent_ref[2, :, cols]
        per_shape = 1.0 / shape_par

        def add_one(m, sums):
            scaled = (maxima_ref[m, :, cols] - loc_par) * per_scale
            inside = 1.0 + shape_par * scaled
            exponent = jnp.log(inside) * per_shape
            rest = 1.0 - jnp.exp(-exponent)
            a = (shape_par + rest) / inside
            sa = scaled * a
            b = sa - 1.0
            c = exponent * rest - sa
            terms = (a, b, c, a * a, a * b, a * c, b * b, b * c, c * c)
            return tuple(s + t for s, t in zip(sums, terms))

        zero = jnp.zeros((8, 256), jnp.float32)
        sums = lax.fori_loop(0, maxima_ref.shape[0], add_one, (zero,) * SUMS, unroll=4)
        ka, kc = 10.0 * per_scale, 0.1 * per_shape
        factors = (ka, None, kc, ka * ka, ka, ka * kc, None, kc, kc * kc)
        sums = [s if k is None else s * k for s, k in zip(sums, factors)]

        owner = swapped(2 * (block // 2) + half)
        for f in range(SUMS):
            for t in range(2):
                at = pl.multiple_of((2 * f + t) * 16 + 8 * (block % 2), 8)
                part_ref[owner, pl.ds(at, 8), :] = sums[f][:, 128 * t : 128 * t + 128]

        def put_edge(to, rows):
            for f in range(SUMS):
                for t in range(2):
                    at = EDGE_AT + (2 * f + t) * HALO
                    part_ref[swapped(to), at : at + HALO, :] = sums[f][rows, 128 * t : 128 * t + 128]

        pl.when(block == 2)(lambda: put_edge(half, slice(0, HALO)))
        pl.when(block == 1)(lambda: put_edge(2 + half, slice(8 - HALO, 8)))

        near = slice(0, 128) if half else slice(128, 256)
        side = pack_sides([s[:, near] for s in sums], bool(half))

        def put_side(to, tile):
            part_ref[swapped(to), pl.ds(pl.multiple_of(SIDE_AT + 8 * tile, 8), 8), :] = side

        pl.when(block <= 2)(lambda: put_side(1 - half, block))
        pl.when(block >= 1)(lambda: put_side(3 - half, block - 1))


def placing(er, ec):
    return dict(
        rows=slice(8, 32) if er == 0 else slice(0, 24),
        cols=slice(128, 512) if ec == 0 else slice(0, 384),
        tile_rows=slice(0, 24) if er == 0 else slice(8, 32),
        tile_cols=slice(0, 384) if ec == 0 else slice(128, 512),
        inner_rows=slice(24, 28) if er == 0 else slice(4, 8),
        outer_rows=slice(4, 8) if er == 0 else slice(24, 28),
        own_edge=slice(8, 12) if er == 0 else slice(20, 24),
        tile_edge=slice(0, 4) if er == 0 else slice(28, 32),
        inner_cols=slice(384, 512) if ec == 0 else slice(0, 128),
        outer_cols=slice(0, 128) if ec == 0 else slice(384, 512),
        own_side=slice(128, 256) if ec == 0 else slice(256, 384),
        tile_side=slice(0, 128) if ec == 0 else slice(384, 512),
        corner=slice(0, 8) if er == 0 else slice(16, 24),
    )


def for_quarter(body):
    mine = swapped(lax.axis_index("ens"))
    for q in range(4):
        pl.when(mine == q)(lambda q=q: body(q // 2, q % 2, placing(q // 2, q % 2)))


def join_kernel(got_ref, latent_ref, precision_ref, window_ref, edge_ref, side_ref, corner_ref):
    def body(er, ec, at):
        def total(start, rows):
            cut = slice(start, start + rows)
            return got_ref[0, cut, :] + got_ref[1, cut, :] + got_ref[2, cut, :] + got_ref[3, cut, :]

        window_ref[...] = jnp.zeros(window_ref.shape, jnp.float32)
        sides = total(SIDE_AT, 24)
        for f in range(SUMS):
            window_ref[f, at["rows"], at["inner_cols"]] = unpack_side(sides, f, ec == 0)
            for t in range(2):
                cols = slice(128 + 128 * t, 256 + 128 * t)
                window_ref[f, 8:24, cols] = total((2 * f + t) * 16, 16)
                window_ref[f, at["inner_rows"], cols] = total(EDGE_AT + (2 * f + t) * HALO, HALO)
        for k, diagonal in enumerate((3, 6, 8)):
            level = precision_ref[k, at["tile_rows"], at["tile_cols"]]
            here = latent_ref[k, at["tile_rows"], at["tile_cols"]]
            there = (at["rows"], at["cols"])
            window_ref[k, *there] = window_ref[k, *there] - level * here
            window_ref[diagonal, *there] = window_ref[diagonal, *there] + level
        for f in range(FIELDS):
            edge_ref[HALO * f : HALO * f + HALO, :] = (
                window_ref[f, at["own_edge"], at["cols"]]
                if f < SUMS
                else latent_ref[f - SUMS, at["tile_edge"], at["tile_cols"]]
            )
        columns = [window_ref[f, at["rows"], at["own_side"]] for f in range(SUMS)]
        columns += [latent_ref[k, at["tile_rows"], at["tile_side"]] for k in range(3)]
        side = pack_sides(columns, ec == 0)
        side_ref[...] = side
        corner_ref[...] = side[at["corner"], :]

    for_quarter(body)


def krylov_kernel(
    coupling_ref, window_ref, latent_ref, edge_ref, side_ref, corner_ref, basis_ref, moments_ref, full_ref
):
    def body(er, ec, at):
        full_ref[0:SUMS] = window_ref[...]
        full_ref[SUMS:FIELDS, at["rows"], at["cols"]] = latent_ref[:, at["tile_rows"], at["tile_cols"]]
        parts = [corner_ref[...], side_ref[...]] if er == 0 else [side_ref[...], corner_ref[...]]
        sides = jnp.concatenate(parts, axis=0)
        for f in range(FIELDS):
            full_ref[f, at["outer_rows"], at["cols"]] = edge_ref[HALO * f : HALO * f + HALO, :]
            full_ref[f, :, at["outer_cols"]] = unpack_side(sides, f, ec == 1)

    for_quarter(body)
    mine = swapped(lax.axis_index("ens"))
    lon = place_of_lon()
    n_lon = lax.axis_size(LON[0]) * lax.axis_size(LON[1])
    shape = (ROWS, COLS)
    row = lax.broadcasted_iota(jnp.int32, shape, 0) + (
        lax.axis_index("lat") * ROWS + 16 * (mine // 2) - 8
    )
    col = lax.broadcasted_iota(jnp.int32, shape, 1) + (lon * COLS + 256 * (mine % 2) - 128)
    inside = (row >= 0) & (row < lax.axis_size("lat") * ROWS) & (col >= 0) & (col < n_lon * COLS)

    def mixed(field):
        laplace = []
        for x in field:
            beside = pltpu.roll(x, 1, 0) + pltpu.roll(x, ROWS - 1, 0)
            beside = beside + (pltpu.roll(x, 1, 1) + pltpu.roll(x, COLS - 1, 1))
            laplace.append(4.0 * x - beside)
        return [
            coupling_ref[k, 0] * laplace[0]
            + coupling_ref[k, 1] * laplace[1]
            + coupling_ref[k, 2] * laplace[2]
            for k in range(3)
        ]

    def operate(field):
        q = mixed(field)
        h = [full_ref[3 + k] for k in range(6)]
        x, y, z = field
        own = (h[0] * x + h[1] * y + h[2] * z, h[1] * x + h[3] * y + h[4] * z, h[2] * x + h[4] * y + h[5] * z)
        return [jnp.where(inside, SCALE * (a + b), 0.0) for a, b in zip(q, own)]

    prior = mixed([full_ref[SUMS + k] for k in range(3)])
    basis = [[jnp.where(inside, full_ref[k] - prior[k], 0.0) for k in range(3)]]
    for _ in range(ITERS):
        basis.append(operate(basis[-1]))
    own = [[x[8:24, 128:384] for x in field] for field in basis]
    for p in range(ITERS):
        for k in range(3):
            basis_ref[3 * p + k] = own[p][k]
    rows = []
    for k in range(2 * ITERS):
        a, b = own[k // 2], own[k - k // 2]
        product = a[0] * b[0] + a[1] * b[1] + a[2] * b[2]
        product = product[:, :128] + product[:, 128:]
        rows.append(jnp.sum(product, axis=0, keepdims=True))
    rows.append(jnp.zeros((2, 128), jnp.float32))
    moments_ref[...] = jnp.broadcast_to(jnp.concatenate(rows, axis=0)[None], moments_ref.shape)


def krylov_weights(m):
    def inner(p, q, shift):
        terms = [p[i] * q[j] * m[i + j + shift] for i in range(len(p)) for j in range(len(q))]
        return sum(terms[1:], terms[0])

    def combine(p, factor, q):
        both = [x + factor * y for x, y in zip(p, q)]
        return both + p[len(q) :] + [factor * y for y in q[len(p) :]]

    one = jnp.ones_like(m[0])
    zero = jnp.zeros_like(m[0])
    weights, residual, direction = [], [one], [one]
    norm_now = m[0]
    for iteration in range(ITERS):
        step_size = norm_now / inner(direction, direction, 1)
        weights = combine(weights, step_size, direction)
        if iteration + 1 < ITERS:
            residual = combine(residual, -step_size, [zero] + direction)
            norm_next = inner(residual, residual, 0)
            direction = combine(residual, norm_next / norm_now, direction)
            norm_now = norm_next
    return [SCALE * w for w in weights]


def update_kernel(moments_ref, latent_ref, *refs):
    basis_refs, solution_ref = refs[:-1], refs[-1]
    moments = jnp.sum(jnp.sum(moments_ref[...], axis=0), axis=1, keepdims=True)
    weights = krylov_weights([moments[k : k + 1, :] for k in range(2 * ITERS)])
    weights = [jnp.broadcast_to(w, (16, 256)) for w in weights]
    mine = lax.axis_index("ens")
    for back, basis_ref in enumerate(basis_refs):
        q = swapped(lax.rem(mine + (4 - back), 4))
        rows = pl.ds(pl.multiple_of(16 * (q // 2), 8), 16)
        cols = pl.ds(pl.multiple_of(256 * (q % 2), 128), 256)
        for k in range(3):
            step = weights[0] * basis_ref[k] + weights[1] * basis_ref[3 + k] + weights[2] * basis_ref[6 + k]
            solution_ref[k, rows, cols] = latent_ref[k, rows, cols] + step


def f32(*shape):
    if INTERPRET:
        return jax.ShapeDtypeStruct(shape, jnp.float32)
    return pltpu.VMEM(shape, jnp.float32)


def near(*arrays):
    if INTERPRET:
        return arrays
    return tuple(pltpu.with_memory_space_constraint(a, pltpu.VMEM) for a in arrays)


def to_neighbour(value, across_lat, across_lon):
    sizes = [lax.axis_size(axis) for axis in EVERY]
    n_lat, n_lon = sizes[1], sizes[2] * sizes[3]
    pairs = []
    for e, lat, lon in itertools.product(range(4), range(n_lat), range(n_lon)):
        lower, right = (e // 2 + lat) % 2, (e + lon) % 2
        lat_to = lat + (2 * lower - 1) * across_lat
        lon_to = lon + (2 * right - 1) * across_lon
        if 0 <= lat_to < n_lat and 0 <= lon_to < n_lon:
            pairs.append(((e * n_lat + lat) * n_lon + lon, (e * n_lat + lat_to) * n_lon + lon_to))
    return lax.ppermute(value, EVERY, pairs)


def per_device(maxima, latent, coupling, local_precision):
    depth = maxima.shape[0]
    part = pl.pallas_call(
        gev_kernel,
        grid=(4,),
        in_specs=[
            pl.BlockSpec((depth, 8, COLS), lambda i: (0, i, 0)),
            pl.BlockSpec((3, 8, COLS), lambda i: (0, i, 0)),
        ],
        out_specs=VMEM,
        out_shape=f32(4, PART_ROWS, 128),
        interpret=INTERPRET,
        name="gev",
    )(maxima, latent)
    got = lax.all_to_all(part, "ens", 0, 0, tiled=True)
    window, edge, side, corner = pl.pallas_call(
        join_kernel,
        in_specs=[VMEM] * 3,
        out_specs=[VMEM] * 4,
        out_shape=[f32(SUMS, ROWS, COLS), f32(FIELDS * HALO, 384), f32(24, 128), f32(8, 128)],
        interpret=INTERPRET,
        name="join",
    )(*near(got), latent, local_precision)
    edge = to_neighbour(edge, 1, 0)
    side = to_neighbour(side, 0, 1)
    corner = to_neighbour(corner, 1, 1)
    n_lat = lax.axis_size("lat")
    basis, moments = pl.pallas_call(
        krylov_kernel,
        in_specs=[SMEM] + [VMEM] * 5,
        out_specs=[VMEM] * 2,
        out_shape=[f32(3 * ITERS, 16, 256), f32(n_lat, 8, 128)],
        scratch_shapes=[pltpu.VMEM((FIELDS, ROWS, COLS), jnp.float32)],
        interpret=INTERPRET,
        name="krylov",
    )(coupling, *near(window), latent, *near(edge, side, corner))
    others = [lax.ppermute(basis, "ens", [(e, (e + k) % 4) for e in range(4)]) for k in range(1, 4)]
    moments = lax.all_to_all(moments, "lat", 0, 0, tiled=True).sum(axis=0)
    rest = ("ens", *LON)
    moments = jnp.broadcast_to(moments, (lax.axis_size(rest), *moments.shape))
    moments = lax.all_to_all(moments, rest, 0, 0, tiled=True)
    return pl.pallas_call(
        update_kernel,
        in_specs=[VMEM] * 6,
        out_specs=VMEM,
        out_shape=jax.ShapeDtypeStruct((3, ROWS, COLS), jnp.float32),
        interpret=INTERPRET,
        name="update",
    )(*near(moments), latent, *near(basis, *others))


def solution(mesh):
    split = Mesh(
        mesh.devices.reshape(mesh.shape["ens"], mesh.shape["lat"], -1, 2),
        ("ens", "lat", "lon_0", "lon_1"),
    )
    placed = (P("ens", "lat", LON), P(None, "lat", LON), P(), P(None, "lat", LON))
    return jax.shard_map(
        per_device, mesh=split, in_specs=placed, out_specs=P(None, "lat", LON), check_vma=False
    )
```

```python
import itertools

import jax
import jax.numpy as jnp
from jax import lax
from jax.experimental import pallas as pl
from jax.experimental.pallas import tpu as pltpu
from jax.sharding import Mesh
from jax.sharding import PartitionSpec as P

ITERS = 3
LON = ("lon_0", "lon_1")
EVERY = ("ens", "lat", *LON)
SCALE = 2.0**-10
LN2 = 0.6931471805599453
INTERPRET = False

ROWS, COLS = 32, 512
SUMS = 9
FIELDS = 12
HALO = 4
EDGE_AT = SUMS * 2 * 16
SIDE_AT = EDGE_AT + SUMS * 2 * HALO
PART_ROWS = SIDE_AT + 24

VMEM = pl.BlockSpec(memory_space=pltpu.VMEM)
SMEM = pl.BlockSpec(memory_space=pltpu.SMEM)


def lanes_of(field, shape):
    lane = lax.broadcasted_iota(jnp.int32, shape, 1)
    return (lane >= HALO * field) & (lane < HALO * (field + 1))


def pack_sides(columns, first):
    packed = jnp.zeros(columns[0].shape, jnp.float32)
    for f, x in enumerate(columns):
        shift = (HALO * f if first else HALO * f + HALO - 128) % 128
        packed = jnp.where(lanes_of(f, x.shape), pltpu.roll(x, shift, 1) if shift else x, packed)
    return packed


def unpack_side(packed, field, first):
    shift = (-HALO * field if first else 128 - HALO - HALO * field) % 128
    return pltpu.roll(packed, shift, 1) if shift else packed


def place_of_lon():
    return lax.axis_index(LON[0]) * lax.axis_size(LON[1]) + lax.axis_index(LON[1])


def swapped(e):
    return 2 * ((e // 2 + lax.axis_index("lat")) % 2) + (e + place_of_lon()) % 2


def gev_kernel(maxima_ref, latent_ref, part_ref):
    block = pl.program_id(0)
    for half in range(2):
        cols = slice(256 * half, 256 * half + 256)
        loc_par = 10.0 * latent_ref[0, :, cols]
        per_scale = jnp.exp(-latent_ref[1, :, cols])
        shape_par = 0.1 * latent_ref[2, :, cols]
        per_shape = -1.0 / (LN2 * shape_par)

        def add_one(m, sums):
            scaled = (maxima_ref[m, :, cols] - loc_par) * per_scale
            inside = 1.0 + shape_par * scaled
            power = jnp.log(inside) * per_shape
            rest = 1.0 - jnp.exp2(power)
            a = (shape_par + rest) / inside
            sa = scaled * a
            b = sa - 1.0
            c = power * rest * -LN2 - sa
            terms = (a, b, c, a * a, a * b, a * c, b * b, b * c, c * c)
            return tuple(s + t for s, t in zip(sums, terms))

        zero = jnp.zeros((8, 256), jnp.float32)
        sums = lax.fori_loop(0, maxima_ref.shape[0], add_one, (zero,) * SUMS, unroll=8)
        ka, kc = 10.0 * per_scale, 0.1 / shape_par
        factors = (ka, None, kc, ka * ka, ka, ka * kc, None, kc, kc * kc)
        sums = [s if k is None else s * k for s, k in zip(sums, factors)]

        owner = swapped(2 * (block // 2) + half)
        for f in range(SUMS):
            for t in range(2):
                at = pl.multiple_of((2 * f + t) * 16 + 8 * (block % 2), 8)
                part_ref[owner, pl.ds(at, 8), :] = sums[f][:, 128 * t : 128 * t + 128]

        def put_edge(to, rows):
            for f in range(SUMS):
                for t in range(2):
                    at = EDGE_AT + (2 * f + t) * HALO
                    part_ref[swapped(to), at : at + HALO, :] = sums[f][rows, 128 * t : 128 * t + 128]

        pl.when(block == 2)(lambda: put_edge(half, slice(0, HALO)))
        pl.when(block == 1)(lambda: put_edge(2 + half, slice(8 - HALO, 8)))

        near = slice(0, 128) if half else slice(128, 256)
        side = pack_sides([s[:, near] for s in sums], bool(half))

        def put_side(to, tile):
            part_ref[swapped(to), pl.ds(pl.multiple_of(SIDE_AT + 8 * tile, 8), 8), :] = side

        pl.when(block <= 2)(lambda: put_side(1 - half, block))
        pl.when(block >= 1)(lambda: put_side(3 - half, block - 1))


def placing(er, ec):
    return dict(
        rows=slice(8, 32) if er == 0 else slice(0, 24),
        cols=slice(128, 512) if ec == 0 else slice(0, 384),
        tile_rows=slice(0, 24) if er == 0 else slice(8, 32),
        tile_cols=slice(0, 384) if ec == 0 else slice(128, 512),
        inner_rows=slice(24, 28) if er == 0 else slice(4, 8),
        outer_rows=slice(4, 8) if er == 0 else slice(24, 28),
        own_edge=slice(8, 12) if er == 0 else slice(20, 24),
        tile_edge=slice(0, 4) if er == 0 else slice(28, 32),
        inner_cols=slice(384, 512) if ec == 0 else slice(0, 128),
        outer_cols=slice(0, 128) if ec == 0 else slice(384, 512),
        own_side=slice(128, 256) if ec == 0 else slice(256, 384),
        tile_side=slice(0, 128) if ec == 0 else slice(384, 512),
        corner=slice(0, 8) if er == 0 else slice(16, 24),
    )


def for_quarter(body):
    mine = swapped(lax.axis_index("ens"))
    for q in range(4):
        pl.when(mine == q)(lambda q=q: body(q // 2, q % 2, placing(q // 2, q % 2)))


def join_kernel(got_ref, latent_ref, precision_ref, window_ref, edge_ref, side_ref, corner_ref):
    def body(er, ec, at):
        def total(start, rows):
            cut = slice(start, start + rows)
            return got_ref[0, cut, :] + got_ref[1, cut, :] + got_ref[2, cut, :] + got_ref[3, cut, :]

        window_ref[...] = jnp.zeros(window_ref.shape, jnp.float32)
        sides = total(SIDE_AT, 24)
        for f in range(SUMS):
            window_ref[f, at["rows"], at["inner_cols"]] = unpack_side(sides, f, ec == 0)
            for t in range(2):
                cols = slice(128 + 128 * t, 256 + 128 * t)
                window_ref[f, 8:24, cols] = total((2 * f + t) * 16, 16)
                window_ref[f, at["inner_rows"], cols] = total(EDGE_AT + (2 * f + t) * HALO, HALO)
        for k, diagonal in enumerate((3, 6, 8)):
            level = precision_ref[k, at["tile_rows"], at["tile_cols"]]
            here = latent_ref[k, at["tile_rows"], at["tile_cols"]]
            there = (at["rows"], at["cols"])
            window_ref[k, *there] = window_ref[k, *there] - level * here
            window_ref[diagonal, *there] = window_ref[diagonal, *there] + level
        for f in range(FIELDS):
            edge_ref[HALO * f : HALO * f + HALO, :] = (
                window_ref[f, at["own_edge"], at["cols"]]
                if f < SUMS
                else latent_ref[f - SUMS, at["tile_edge"], at["tile_cols"]]
            )
        columns = [window_ref[f, at["rows"], at["own_side"]] for f in range(SUMS)]
        columns += [latent_ref[k, at["tile_rows"], at["tile_side"]] for k in range(3)]
        side = pack_sides(columns, ec == 0)
        side_ref[...] = side
        corner_ref[...] = side[at["corner"], :]

    for_quarter(body)


def krylov_kernel(
    coupling_ref, window_ref, latent_ref, edge_ref, side_ref, corner_ref, basis_ref, moments_ref, full_ref
):
    def body(er, ec, at):
        full_ref[0:SUMS] = window_ref[...]
        full_ref[SUMS:FIELDS, at["rows"], at["cols"]] = latent_ref[:, at["tile_rows"], at["tile_cols"]]
        parts = [corner_ref[...], side_ref[...]] if er == 0 else [side_ref[...], corner_ref[...]]
        sides = jnp.concatenate(parts, axis=0)
        for f in range(FIELDS):
            full_ref[f, at["outer_rows"], at["cols"]] = edge_ref[HALO * f : HALO * f + HALO, :]
            full_ref[f, :, at["outer_cols"]] = unpack_side(sides, f, ec == 1)

    for_quarter(body)
    mine = swapped(lax.axis_index("ens"))
    lon = place_of_lon()
    n_lon = lax.axis_size(LON[0]) * lax.axis_size(LON[1])
    shape = (ROWS, COLS)
    row = lax.broadcasted_iota(jnp.int32, shape, 0) + (
        lax.axis_index("lat") * ROWS + 16 * (mine // 2) - 8
    )
    col = lax.broadcasted_iota(jnp.int32, shape, 1) + (lon * COLS + 256 * (mine % 2) - 128)
    inside = (row >= 0) & (row < lax.axis_size("lat") * ROWS) & (col >= 0) & (col < n_lon * COLS)

    def mixed(field):
        laplace = []
        for x in field:
            beside = pltpu.roll(x, 1, 0) + pltpu.roll(x, ROWS - 1, 0)
            beside = beside + (pltpu.roll(x, 1, 1) + pltpu.roll(x, COLS - 1, 1))
            laplace.append(4.0 * x - beside)
        return [
            coupling_ref[k, 0] * laplace[0]
            + coupling_ref[k, 1] * laplace[1]
            + coupling_ref[k, 2] * laplace[2]
            for k in range(3)
        ]

    def operate(field):
        q = mixed(field)
        h = [full_ref[3 + k] for k in range(6)]
        x, y, z = field
        own = (h[0] * x + h[1] * y + h[2] * z, h[1] * x + h[3] * y + h[4] * z, h[2] * x + h[4] * y + h[5] * z)
        return [jnp.where(inside, SCALE * (a + b), 0.0) for a, b in zip(q, own)]

    prior = mixed([full_ref[SUMS + k] for k in range(3)])
    basis = [[jnp.where(inside, full_ref[k] - prior[k], 0.0) for k in range(3)]]
    for _ in range(ITERS):
        basis.append(operate(basis[-1]))
    own = [[x[8:24, 128:384] for x in field] for field in basis]
    for p in range(ITERS):
        for k in range(3):
            basis_ref[3 * p + k] = own[p][k]
    lane = lax.broadcasted_iota(jnp.int32, (1, 128), 1)
    moments = jnp.zeros((1, 128), jnp.float32)
    for k in range(2 * ITERS):
        a, b = own[k // 2], own[k - k // 2]
        product = a[0] * b[0] + a[1] * b[1] + a[2] * b[2]
        total = jnp.sum(jnp.sum(product, axis=0, keepdims=True), axis=1, keepdims=True)
        moments = jnp.where(lane == k, total, moments)
    moments_ref[...] = jnp.broadcast_to(moments[None], moments_ref.shape)


def krylov_weights(m):
    def inner(p, q, shift):
        terms = [p[i] * q[j] * m[i + j + shift] for i in range(len(p)) for j in range(len(q))]
        return sum(terms[1:], terms[0])

    def combine(p, factor, q):
        both = [x + factor * y for x, y in zip(p, q)]
        return both + p[len(q) :] + [factor * y for y in q[len(p) :]]

    one = jnp.ones_like(m[0])
    zero = jnp.zeros_like(m[0])
    weights, residual, direction = [], [one], [one]
    norm_now = m[0]
    for iteration in range(ITERS):
        step_size = norm_now / inner(direction, direction, 1)
        weights = combine(weights, step_size, direction)
        if iteration + 1 < ITERS:
            residual = combine(residual, -step_size, [zero] + direction)
            norm_next = inner(residual, residual, 0)
            direction = combine(residual, norm_next / norm_now, direction)
            norm_now = norm_next
    return [SCALE * w for w in weights]


def update_kernel(moments_ref, latent_ref, *refs):
    basis_refs, solution_ref = refs[:-1], refs[-1]
    moments = jnp.sum(moments_ref[...], axis=0)
    moments = [jnp.broadcast_to(moments[:, k : k + 1], (8, 128)) for k in range(2 * ITERS)]
    weights = [jnp.tile(w, (2, 2)) for w in krylov_weights(moments)]
    mine = lax.axis_index("ens")
    for back, basis_ref in enumerate(basis_refs):
        q = swapped(lax.rem(mine + (4 - back), 4))
        rows = pl.ds(pl.multiple_of(16 * (q // 2), 8), 16)
        cols = pl.ds(pl.multiple_of(256 * (q % 2), 128), 256)
        for k in range(3):
            step = weights[0] * basis_ref[k] + weights[1] * basis_ref[3 + k] + weights[2] * basis_ref[6 + k]
            solution_ref[k, rows, cols] = latent_ref[k, rows, cols] + step


def f32(*shape):
    if INTERPRET:
        return jax.ShapeDtypeStruct(shape, jnp.float32)
    return pltpu.VMEM(shape, jnp.float32)


def near(*arrays):
    if INTERPRET:
        return arrays
    return tuple(pltpu.with_memory_space_constraint(a, pltpu.VMEM) for a in arrays)


def to_neighbour(value, across_lat, across_lon):
    sizes = [lax.axis_size(axis) for axis in EVERY]
    n_lat, n_lon = sizes[1], sizes[2] * sizes[3]
    pairs = []
    for e, lat, lon in itertools.product(range(4), range(n_lat), range(n_lon)):
        lower, right = (e // 2 + lat) % 2, (e + lon) % 2
        lat_to = lat + (2 * lower - 1) * across_lat
        lon_to = lon + (2 * right - 1) * across_lon
        if 0 <= lat_to < n_lat and 0 <= lon_to < n_lon:
            pairs.append(((e * n_lat + lat) * n_lon + lon, (e * n_lat + lat_to) * n_lon + lon_to))
    return lax.ppermute(value, EVERY, pairs)


def per_device(maxima, latent, coupling, local_precision):
    depth = maxima.shape[0]
    part = pl.pallas_call(
        gev_kernel,
        grid=(4,),
        in_specs=[
            pl.BlockSpec((depth, 8, COLS), lambda i: (0, i, 0)),
            pl.BlockSpec((3, 8, COLS), lambda i: (0, i, 0)),
        ],
        out_specs=VMEM,
        out_shape=f32(4, PART_ROWS, 128),
        interpret=INTERPRET,
        name="gev",
    )(maxima, latent)
    got = lax.all_to_all(part, "ens", 0, 0, tiled=True)
    window, edge, side, corner = pl.pallas_call(
        join_kernel,
        in_specs=[VMEM] * 3,
        out_specs=[VMEM] * 4,
        out_shape=[f32(SUMS, ROWS, COLS), f32(FIELDS * HALO, 384), f32(24, 128), f32(8, 128)],
        interpret=INTERPRET,
        name="join",
    )(*near(got, latent, local_precision))
    edge = to_neighbour(edge, 1, 0)
    side = to_neighbour(side, 0, 1)
    corner = to_neighbour(corner, 1, 1)
    n_lat = lax.axis_size("lat")
    basis, moments = pl.pallas_call(
        krylov_kernel,
        in_specs=[SMEM] + [VMEM] * 5,
        out_specs=[VMEM] * 2,
        out_shape=[f32(3 * ITERS, 16, 256), f32(n_lat, 1, 128)],
        scratch_shapes=[pltpu.VMEM((FIELDS, ROWS, COLS), jnp.float32)],
        interpret=INTERPRET,
        name="krylov",
    )(coupling, *near(window, latent, edge, side, corner))

    def from_back(values, back):
        return lax.ppermute(values, "ens", [(e, (e + back) % 4) for e in range(4)])

    moments = lax.all_to_all(moments, "lat", 0, 0, tiled=True).sum(axis=0)
    later, moments = lax.optimization_barrier((basis, moments))
    others = [from_back(basis, 1), from_back(later, 2), from_back(basis, 3)]
    rest = ("ens", *LON)
    moments = jnp.broadcast_to(moments, (lax.axis_size(rest), *moments.shape))
    moments = lax.all_to_all(moments, rest, 0, 0, tiled=True)
    return pl.pallas_call(
        update_kernel,
        in_specs=[VMEM] * 6,
        out_specs=VMEM,
        out_shape=jax.ShapeDtypeStruct((3, ROWS, COLS), jnp.float32),
        interpret=INTERPRET,
        name="update",
    )(*near(moments, latent, basis, *others))


def solution(mesh):
    split = Mesh(
        mesh.devices.reshape(mesh.shape["ens"], mesh.shape["lat"], -1, 2),
        ("ens", "lat", "lon_0", "lon_1"),
    )
    placed = (P("ens", "lat", LON), P(None, "lat", LON), P(), P(None, "lat", LON))
    return jax.shard_map(
        per_device, mesh=split, in_specs=placed, out_specs=P(None, "lat", LON), check_vma=False
    )
```

```python
import itertools

import jax
import jax.numpy as jnp
from jax import lax
from jax.experimental import pallas as pl
from jax.experimental.pallas import tpu as pltpu
from jax.sharding import Mesh
from jax.sharding import PartitionSpec as P


ITERS = 3
LON = ("lon_0", "lon_1")
EVERY = ("ens", "lat", *LON)
SCALE = 2.0**-10
LN2 = 0.6931471805599453
INTERPRET = False

ROWS, COLS = 32, 512
SUMS = 9
FIELDS = 12
HALO = 4
DEPTH = (3,) * 3 + (2,) * 6 + (4,) * 3
ABOVE = [sum(DEPTH[:f]) for f in range(FIELDS)]
EDGE_AT = SUMS * 2 * 16
SIDE_AT = EDGE_AT + 48
PART_ROWS = SIDE_AT + 24
BLOCK = 40
BEND_AT = 2 * BLOCK
EDGE_ROWS = BEND_AT + 8

VMEM = pl.BlockSpec(memory_space=pltpu.VMEM)
SMEM = pl.BlockSpec(memory_space=pltpu.SMEM)


def lanes_of(field, shape):
    lane = lax.broadcasted_iota(jnp.int32, shape, 1)
    return (lane >= HALO * field) & (lane < HALO * (field + 1))


def pack_sides(columns, first):
    packed = jnp.zeros(columns[0].shape, jnp.float32)
    for f, x in enumerate(columns):
        shift = (HALO * f if first else HALO * f + HALO - 128) % 128
        packed = jnp.where(lanes_of(f, x.shape), pltpu.roll(x, shift, 1) if shift else x, packed)
    return packed


def unpack_side(packed, field, first):
    shift = (-HALO * field if first else 128 - HALO - HALO * field) % 128
    return pltpu.roll(packed, shift, 1) if shift else packed


def place_of_lon():
    return lax.axis_index(LON[0]) * lax.axis_size(LON[1]) + lax.axis_index(LON[1])


def swapped(e):
    return 2 * ((e // 2 + lax.axis_index("lat")) % 2) + (e + place_of_lon()) % 2


def gev_kernel(maxima_ref, latent_ref, part_ref):
    block = pl.program_id(0)
    for half in range(2):
        cols = slice(256 * half, 256 * half + 256)
        loc_par = 10.0 * latent_ref[0, :, cols]
        per_scale = jnp.exp(-latent_ref[1, :, cols])
        shape_par = 0.1 * latent_ref[2, :, cols]
        per_shape = -1.0 / (LN2 * shape_par)

        def add_one(m, sums):
            scaled = (maxima_ref[m, :, cols] - loc_par) * per_scale
            inside = 1.0 + shape_par * scaled
            power = jnp.log(inside) * per_shape
            rest = 1.0 - jnp.exp2(power)
            a = (shape_par + rest) / inside
            sa = scaled * a
            b = sa - 1.0
            c = power * rest * -LN2 - sa
            terms = (a, b, c, a * a, a * b, a * c, b * b, b * c, c * c)
            return tuple(s + t for s, t in zip(sums, terms))

        zero = jnp.zeros((8, 256), jnp.float32)
        sums = lax.fori_loop(0, maxima_ref.shape[0], add_one, (zero,) * SUMS, unroll=8)
        ka, kc = 10.0 * per_scale, 0.1 / shape_par
        factors = (ka, None, kc, ka * ka, ka, ka * kc, None, kc, kc * kc)
        sums = [s if k is None else s * k for s, k in zip(sums, factors)]

        owner = swapped(2 * (block // 2) + half)
        for f in range(SUMS):
            for t in range(2):
                at = pl.multiple_of((2 * f + t) * 16 + 8 * (block % 2), 8)
                part_ref[owner, pl.ds(at, 8), :] = sums[f][:, 128 * t : 128 * t + 128]

        def put_edge(to, top):
            for f in range(SUMS):
                rows = slice(0, DEPTH[f]) if top else slice(8 - DEPTH[f], 8)
                for t in range(2):
                    at = EDGE_AT + 24 * t + ABOVE[f]
                    part_ref[swapped(to), at : at + DEPTH[f], :] = sums[f][rows, 128 * t : 128 * t + 128]

        pl.when(block == 2)(lambda: put_edge(half, True))
        pl.when(block == 1)(lambda: put_edge(2 + half, False))

        near = slice(0, 128) if half else slice(128, 256)
        side = pack_sides([s[:, near] for s in sums], bool(half))

        def put_side(to, tile):
            part_ref[swapped(to), pl.ds(pl.multiple_of(SIDE_AT + 8 * tile, 8), 8), :] = side

        pl.when(block <= 2)(lambda: put_side(1 - half, block))
        pl.when(block >= 1)(lambda: put_side(3 - half, block - 1))


def placing(er, ec):
    return dict(
        rows=slice(8, 32) if er == 0 else slice(0, 24),
        cols=slice(128, 512) if ec == 0 else slice(0, 384),
        tile_rows=slice(0, 24) if er == 0 else slice(8, 32),
        tile_cols=slice(0, 384) if ec == 0 else slice(128, 512),
        inner_rows=[slice(24, 24 + d) if er == 0 else slice(8 - d, 8) for d in DEPTH],
        outer_rows=[slice(8 - d, 8) if er == 0 else slice(24, 24 + d) for d in DEPTH],
        outer_tile=slice(0, 8) if er == 0 else slice(24, 32),
        own_edge=[slice(8, 8 + d) if er == 0 else slice(24 - d, 24) for d in DEPTH],
        own_tile=slice(8, 16) if er == 0 else slice(16, 24),
        tile_edge=slice(0, HALO) if er == 0 else slice(32 - HALO, 32),
        tile_tile=slice(0, 8) if er == 0 else slice(24, 32),
        tile_inner=slice(256, 384) if ec == 0 else slice(128, 256),
        inner_cols=slice(384, 512) if ec == 0 else slice(0, 128),
        outer_cols=slice(0, 128) if ec == 0 else slice(384, 512),
        own_side=slice(128, 256) if ec == 0 else slice(256, 384),
        tile_side=slice(0, 128) if ec == 0 else slice(384, 512),
        corner=slice(0, 8) if er == 0 else slice(16, 24),
    )


def for_quarter(body):
    mine = swapped(lax.axis_index("ens"))
    for q in range(4):
        pl.when(mine == q)(lambda q=q: body(q // 2, q % 2, placing(q // 2, q % 2)))


def join_kernel(got_ref, latent_ref, precision_ref, window_ref, send_ref):
    def body(er, ec, at):
        def total(start, rows):
            cut = slice(start, start + rows)
            return got_ref[0, cut, :] + got_ref[1, cut, :] + got_ref[2, cut, :] + got_ref[3, cut, :]

        window_ref[...] = jnp.zeros(window_ref.shape, jnp.float32)
        sides = total(SIDE_AT, 24)
        for f in range(SUMS):
            window_ref[f, at["rows"], at["inner_cols"]] = unpack_side(sides, f, ec == 0)
            for t in range(2):
                cols = slice(128 + 128 * t, 256 + 128 * t)
                window_ref[f, 8:24, cols] = total((2 * f + t) * 16, 16)
                window_ref[f, at["inner_rows"][f], cols] = total(EDGE_AT + 24 * t + ABOVE[f], DEPTH[f])
        for k, diagonal in enumerate((3, 6, 8)):
            level = precision_ref[k, at["tile_rows"], at["tile_cols"]]
            here = latent_ref[k, at["tile_rows"], at["tile_cols"]]
            there = (at["rows"], at["cols"])
            window_ref[k, *there] = window_ref[k, *there] - level * here
            window_ref[diagonal, *there] = window_ref[diagonal, *there] + level
        over = 2 * (1 - er) + ec
        for f in range(FIELDS):
            for t in range(2):
                rows = slice(BLOCK * t + ABOVE[f], BLOCK * t + ABOVE[f] + DEPTH[f])
                tile_cols = slice(256 * ec + 128 * t, 256 * ec + 128 * t + 128)
                send_ref[over, rows, :] = (
                    window_ref[f, at["own_edge"][f], 128 + 128 * t : 256 + 128 * t]
                    if f < SUMS
                    else latent_ref[f - SUMS, at["tile_edge"], tile_cols]
                )
        columns = [window_ref[f, at["own_tile"], at["inner_cols"]] for f in range(SUMS)]
        columns += [latent_ref[k, at["tile_tile"], at["tile_inner"]] for k in range(3)]
        send_ref[over, BEND_AT:EDGE_ROWS, :] = pack_sides(columns, ec == 0)
        columns = [window_ref[f, at["rows"], at["own_side"]] for f in range(SUMS)]
        columns += [latent_ref[k, at["tile_rows"], at["tile_side"]] for k in range(3)]
        side = pack_sides(columns, ec == 0)
        send_ref[2 * er + 1 - ec, 0:24, :] = side
        send_ref[3 - 2 * er - ec, 0:8, :] = side[at["corner"], :]

    for_quarter(body)


def krylov_kernel(
    coupling_ref, window_ref, latent_ref, got_ref, basis_ref, moments_ref, full_ref
):
    def body(er, ec, at):
        full_ref[0:SUMS] = window_ref[...]
        full_ref[SUMS:FIELDS, at["rows"], at["cols"]] = latent_ref[:, at["tile_rows"], at["tile_cols"]]
        side, corner = got_ref[2 * er + 1 - ec, 0:24, :], got_ref[3 - 2 * er - ec, 0:8, :]
        parts = [corner, side] if er == 0 else [side, corner]
        sides = jnp.concatenate(parts, axis=0)
        over = 2 * (1 - er) + ec
        bend = got_ref[over, BEND_AT:EDGE_ROWS, :]
        for f in range(FIELDS):
            for t in range(2):
                rows = slice(BLOCK * t + ABOVE[f], BLOCK * t + ABOVE[f] + DEPTH[f])
                full_ref[f, at["outer_rows"][f], 128 + 128 * t : 256 + 128 * t] = got_ref[over, rows, :]
            full_ref[f, at["outer_tile"], at["inner_cols"]] = unpack_side(bend, f, ec == 0)
            full_ref[f, :, at["outer_cols"]] = unpack_side(sides, f, ec == 1)

    for_quarter(body)
    mine = swapped(lax.axis_index("ens"))
    lon = place_of_lon()
    n_lon = lax.axis_size(LON[0]) * lax.axis_size(LON[1])
    shape = (ROWS, COLS)
    row = lax.broadcasted_iota(jnp.int32, shape, 0) + (
        lax.axis_index("lat") * ROWS + 16 * (mine // 2) - 8
    )
    col = lax.broadcasted_iota(jnp.int32, shape, 1) + (lon * COLS + 256 * (mine % 2) - 128)
    inside = (row >= 0) & (row < lax.axis_size("lat") * ROWS) & (col >= 0) & (col < n_lon * COLS)

    def mixed(field):
        laplace = []
        for x in field:
            beside = pltpu.roll(x, 1, 0) + pltpu.roll(x, ROWS - 1, 0)
            beside = beside + (pltpu.roll(x, 1, 1) + pltpu.roll(x, COLS - 1, 1))
            laplace.append(4.0 * x - beside)
        return [
            coupling_ref[k, 0] * laplace[0]
            + coupling_ref[k, 1] * laplace[1]
            + coupling_ref[k, 2] * laplace[2]
            for k in range(3)
        ]

    def operate(field):
        q = mixed(field)
        h = [full_ref[3 + k] for k in range(6)]
        x, y, z = field
        own = (h[0] * x + h[1] * y + h[2] * z, h[1] * x + h[3] * y + h[4] * z, h[2] * x + h[4] * y + h[5] * z)
        return [jnp.where(inside, SCALE * (a + b), 0.0) for a, b in zip(q, own)]

    prior = mixed([jnp.where(inside, full_ref[SUMS + k], 0.0) for k in range(3)])
    basis = [[jnp.where(inside, full_ref[k] - prior[k], 0.0) for k in range(3)]]
    for _ in range(ITERS):
        basis.append(operate(basis[-1]))
    own = [[x[8:24, 128:384] for x in field] for field in basis]
    for p in range(ITERS):
        for k in range(3):
            basis_ref[3 * p + k] = own[p][k]
    lane = lax.broadcasted_iota(jnp.int32, (1, 128), 1)
    moments = jnp.zeros((1, 128), jnp.float32)
    for k in range(2 * ITERS):
        a, b = own[k // 2], own[k - k // 2]
        product = a[0] * b[0] + a[1] * b[1] + a[2] * b[2]
        total = jnp.sum(jnp.sum(product, axis=0, keepdims=True), axis=1, keepdims=True)
        moments = jnp.where(lane == k, total, moments)
    moments_ref[...] = jnp.broadcast_to(moments[None], moments_ref.shape)


def krylov_weights(m):
    def inner(p, q, shift):
        terms = [p[i] * q[j] * m[i + j + shift] for i in range(len(p)) for j in range(len(q))]
        return sum(terms[1:], terms[0])

    def combine(p, factor, q):
        both = [x + factor * y for x, y in zip(p, q)]
        return both + p[len(q) :] + [factor * y for y in q[len(p) :]]

    one = jnp.ones_like(m[0])
    zero = jnp.zeros_like(m[0])
    weights, residual, direction = [], [one], [one]
    norm_now = m[0]
    for iteration in range(ITERS):
        step_size = norm_now / inner(direction, direction, 1)
        weights = combine(weights, step_size, direction)
        if iteration + 1 < ITERS:
            residual = combine(residual, -step_size, [zero] + direction)
            norm_next = inner(residual, residual, 0)
            direction = combine(residual, norm_next / norm_now, direction)
            norm_now = norm_next
    return [SCALE * w for w in weights]


def update_kernel(moments_ref, latent_ref, *refs):
    basis_refs, solution_ref = refs[:-1], refs[-1]
    moments = jnp.sum(moments_ref[...], axis=0)
    moments = [jnp.broadcast_to(moments[:, k : k + 1], (8, 128)) for k in range(2 * ITERS)]
    weights = [jnp.tile(w, (2, 2)) for w in krylov_weights(moments)]
    mine = lax.axis_index("ens")
    for back, basis_ref in zip((0, 2, 1, 3), basis_refs):
        q = swapped(lax.rem(mine + (4 - back), 4))
        rows = pl.ds(pl.multiple_of(16 * (q // 2), 8), 16)
        cols = pl.ds(pl.multiple_of(256 * (q % 2), 128), 256)
        for k in range(3):
            step = weights[0] * basis_ref[k] + weights[1] * basis_ref[3 + k] + weights[2] * basis_ref[6 + k]
            solution_ref[k, rows, cols] = latent_ref[k, rows, cols] + step


def f32(*shape):
    if INTERPRET:
        return jax.ShapeDtypeStruct(shape, jnp.float32)
    return pltpu.VMEM(shape, jnp.float32)


def near(*arrays):
    if INTERPRET:
        return arrays
    return tuple(pltpu.with_memory_space_constraint(a, pltpu.VMEM) for a in arrays)


def around_vertices():
    sizes = [lax.axis_size(axis) for axis in EVERY]
    n_lat, n_lon = sizes[1], sizes[2] * sizes[3]
    groups = {}
    for e, lat, lon in itertools.product(range(4), range(n_lat), range(n_lon)):
        lower, right = (e // 2 + lat) % 2, (e + lon) % 2
        vertex = (e, (lat + lower) % n_lat, (lon + right) % n_lon)
        groups.setdefault(vertex, {})[2 * lower + right] = (e * n_lat + lat) * n_lon + lon
    return [[group[q] for q in range(4)] for group in groups.values()]


def per_device(maxima, latent, coupling, local_precision):
    depth = maxima.shape[0]
    part = pl.pallas_call(
        gev_kernel,
        grid=(4,),
        in_specs=[
            pl.BlockSpec((depth, 8, COLS), lambda i: (0, i, 0)),
            pl.BlockSpec((3, 8, COLS), lambda i: (0, i, 0)),
        ],
        out_specs=VMEM,
        out_shape=f32(4, PART_ROWS, 128),
        interpret=INTERPRET,
        name="gev",
    )(maxima, latent)
    got = lax.all_to_all(part, "ens", 0, 0, tiled=True)
    window, halo = pl.pallas_call(
        join_kernel,
        in_specs=[VMEM] * 3,
        out_specs=[VMEM] * 2,
        out_shape=[f32(SUMS, ROWS, COLS), f32(4, EDGE_ROWS, 128)],
        interpret=INTERPRET,
        name="join",
    )(*near(got, latent, local_precision))
    halo = lax.all_to_all(halo, EVERY, 0, 0, axis_index_groups=around_vertices(), tiled=True)
    n_lat = lax.axis_size("lat")
    basis, moments = pl.pallas_call(
        krylov_kernel,
        in_specs=[SMEM] + [VMEM] * 3,
        out_specs=[VMEM] * 2,
        out_shape=[f32(3 * ITERS, 16, 256), f32(n_lat, 1, 128)],
        scratch_shapes=[pltpu.VMEM((FIELDS, ROWS, COLS), jnp.float32)],
        interpret=INTERPRET,
        name="krylov",
    )(coupling, *near(window, latent, halo))

    def from_back(values, back):
        return lax.ppermute(values, "ens", [(e, (e + back) % 4) for e in range(4)])

    moments = lax.all_to_all(moments, "lat", 0, 0, tiled=True)
    moments = moments.sum(axis=0)
    others = []
    for back in (2, 1, 3):
        others.append(from_back(basis, back))
    rest = ("ens", *LON)
    moments = jnp.broadcast_to(moments, (lax.axis_size(rest), *moments.shape))
    moments = lax.all_to_all(moments, rest, 0, 0, tiled=True)
    return pl.pallas_call(
        update_kernel,
        in_specs=[VMEM] * 6,
        out_specs=VMEM,
        out_shape=jax.ShapeDtypeStruct((3, ROWS, COLS), jnp.float32),
        interpret=INTERPRET,
        name="update",
    )(*near(moments, latent, basis, *others))


def solution(mesh):
    split = Mesh(
        mesh.devices.reshape(mesh.shape["ens"], mesh.shape["lat"], -1, 2),
        ("ens", "lat", "lon_0", "lon_1"),
    )
    placed = (P("ens", "lat", LON), P(None, "lat", LON), P(), P(None, "lat", LON))
    return jax.shard_map(
        per_device, mesh=split, in_specs=placed, out_specs=P(None, "lat", LON), check_vma=False
    )
```

```python
import itertools

import jax
import jax.numpy as jnp
from jax import lax
from jax.experimental import pallas as pl
from jax.experimental.pallas import tpu as pltpu
from jax.sharding import Mesh
from jax.sharding import PartitionSpec as P


ITERS = 3
LON = ("lon_0", "lon_1")
EVERY = ("ens", "lat", *LON)
SCALE = 2.0**-10
LN2 = 0.6931471805599453
INTERPRET = False

ROWS, COLS = 32, 512
SUMS = 9
FIELDS = 12
HALO = 4
DEPTH = (3,) * 3 + (2,) * 6 + (4,) * 3
ABOVE = [sum(DEPTH[:f]) for f in range(FIELDS)]
EDGE_AT = SUMS * 2 * 16
SIDE_AT = EDGE_AT + 48
PART_ROWS = SIDE_AT + 24
BLOCK = 40
BEND_AT = 2 * BLOCK
EDGE_ROWS = BEND_AT + 8

VMEM = pl.BlockSpec(memory_space=pltpu.VMEM)


def lanes_of(field, shape):
    lane = lax.broadcasted_iota(jnp.int32, shape, 1)
    return (lane >= HALO * field) & (lane < HALO * (field + 1))


def pack_sides(columns, first):
    packed = jnp.zeros(columns[0].shape, jnp.float32)
    for f, x in enumerate(columns):
        shift = (HALO * f if first else HALO * f + HALO - 128) % 128
        packed = jnp.where(lanes_of(f, x.shape), pltpu.roll(x, shift, 1) if shift else x, packed)
    return packed


def unpack_side(packed, field, first):
    shift = (-HALO * field if first else 128 - HALO - HALO * field) % 128
    return pltpu.roll(packed, shift, 1) if shift else packed


def place_of_lon():
    return lax.axis_index(LON[0]) * lax.axis_size(LON[1]) + lax.axis_index(LON[1])


def swapped(e):
    return 2 * ((e // 2 + lax.axis_index("lat")) % 2) + (e + place_of_lon()) % 2


def gev_kernel(maxima_ref, latent_ref, part_ref):
    block = pl.program_id(0)
    for half in range(2):
        cols = slice(256 * half, 256 * half + 256)
        loc_par = 10.0 * latent_ref[0, :, cols]
        per_scale = jnp.exp(-latent_ref[1, :, cols])
        shape_par = 0.1 * latent_ref[2, :, cols]
        per_shape = -1.0 / (LN2 * shape_par)

        def add_one(m, sums):
            scaled = (maxima_ref[m, :, cols] - loc_par) * per_scale
            inside = 1.0 + shape_par * scaled
            power = jnp.log(inside) * per_shape
            rest = 1.0 - jnp.exp2(power)
            a = (shape_par + rest) / inside
            sa = scaled * a
            b = sa - 1.0
            c = power * rest * -LN2 - sa
            terms = (a, b, c, a * a, a * b, a * c, b * b, b * c, c * c)
            return tuple(s + t for s, t in zip(sums, terms))

        zero = jnp.zeros((8, 256), jnp.float32)
        sums = lax.fori_loop(0, maxima_ref.shape[0], add_one, (zero,) * SUMS, unroll=8)
        ka, kc = 10.0 * per_scale, 0.1 / shape_par
        factors = (ka, None, kc, ka * ka, ka, ka * kc, None, kc, kc * kc)
        sums = [s if k is None else s * k for s, k in zip(sums, factors)]

        owner = swapped(2 * (block // 2) + half)
        for f in range(SUMS):
            for t in range(2):
                at = pl.multiple_of((2 * f + t) * 16 + 8 * (block % 2), 8)
                part_ref[owner, pl.ds(at, 8), :] = sums[f][:, 128 * t : 128 * t + 128]

        def put_edge(to, top):
            for f in range(SUMS):
                rows = slice(0, DEPTH[f]) if top else slice(8 - DEPTH[f], 8)
                for t in range(2):
                    at = EDGE_AT + 24 * t + ABOVE[f]
                    part_ref[swapped(to), at : at + DEPTH[f], :] = sums[f][rows, 128 * t : 128 * t + 128]

        pl.when(block == 2)(lambda: put_edge(half, True))
        pl.when(block == 1)(lambda: put_edge(2 + half, False))

        near = slice(0, 128) if half else slice(128, 256)
        side = pack_sides([s[:, near] for s in sums], bool(half))

        def put_side(to, tile):
            part_ref[swapped(to), pl.ds(pl.multiple_of(SIDE_AT + 8 * tile, 8), 8), :] = side

        pl.when(block <= 2)(lambda: put_side(1 - half, block))
        pl.when(block >= 1)(lambda: put_side(3 - half, block - 1))


def placing(er, ec):
    return dict(
        rows=slice(8, 32) if er == 0 else slice(0, 24),
        cols=slice(128, 512) if ec == 0 else slice(0, 384),
        tile_rows=slice(0, 24) if er == 0 else slice(8, 32),
        tile_cols=slice(0, 384) if ec == 0 else slice(128, 512),
        inner_rows=[slice(24, 24 + d) if er == 0 else slice(8 - d, 8) for d in DEPTH],
        outer_rows=[slice(8 - d, 8) if er == 0 else slice(24, 24 + d) for d in DEPTH],
        outer_tile=slice(0, 8) if er == 0 else slice(24, 32),
        own_edge=[slice(8, 8 + d) if er == 0 else slice(24 - d, 24) for d in DEPTH],
        own_tile=slice(8, 16) if er == 0 else slice(16, 24),
        tile_edge=slice(0, HALO) if er == 0 else slice(32 - HALO, 32),
        tile_tile=slice(0, 8) if er == 0 else slice(24, 32),
        tile_inner=slice(256, 384) if ec == 0 else slice(128, 256),
        inner_cols=slice(384, 512) if ec == 0 else slice(0, 128),
        outer_cols=slice(0, 128) if ec == 0 else slice(384, 512),
        own_side=slice(128, 256) if ec == 0 else slice(256, 384),
        tile_side=slice(0, 128) if ec == 0 else slice(384, 512),
        corner=slice(0, 8) if er == 0 else slice(16, 24),
    )


def for_quarter(body):
    mine = swapped(lax.axis_index("ens"))
    for q in range(4):
        pl.when(mine == q)(lambda q=q: body(q // 2, q % 2, placing(q // 2, q % 2)))


def join_kernel(got_ref, latent_ref, precision_ref, window_ref, send_ref):
    def body(er, ec, at):
        def total(start, rows):
            cut = slice(start, start + rows)
            return got_ref[0, cut, :] + got_ref[1, cut, :] + got_ref[2, cut, :] + got_ref[3, cut, :]

        window_ref[...] = jnp.zeros(window_ref.shape, jnp.float32)
        sides = total(SIDE_AT, 24)
        for f in range(SUMS):
            window_ref[f, at["rows"], at["inner_cols"]] = unpack_side(sides, f, ec == 0)
            for t in range(2):
                cols = slice(128 + 128 * t, 256 + 128 * t)
                window_ref[f, 8:24, cols] = total((2 * f + t) * 16, 16)
                window_ref[f, at["inner_rows"][f], cols] = total(EDGE_AT + 24 * t + ABOVE[f], DEPTH[f])
        for k, diagonal in enumerate((3, 6, 8)):
            level = precision_ref[k, at["tile_rows"], at["tile_cols"]]
            here = latent_ref[k, at["tile_rows"], at["tile_cols"]]
            there = (at["rows"], at["cols"])
            window_ref[k, *there] = window_ref[k, *there] - level * here
            window_ref[diagonal, *there] = window_ref[diagonal, *there] + level
        over = 2 * (1 - er) + ec
        for f in range(FIELDS):
            for t in range(2):
                rows = slice(BLOCK * t + ABOVE[f], BLOCK * t + ABOVE[f] + DEPTH[f])
                tile_cols = slice(256 * ec + 128 * t, 256 * ec + 128 * t + 128)
                send_ref[over, rows, :] = (
                    window_ref[f, at["own_edge"][f], 128 + 128 * t : 256 + 128 * t]
                    if f < SUMS
                    else latent_ref[f - SUMS, at["tile_edge"], tile_cols]
                )
        columns = [window_ref[f, at["own_tile"], at["inner_cols"]] for f in range(SUMS)]
        columns += [latent_ref[k, at["tile_tile"], at["tile_inner"]] for k in range(3)]
        send_ref[over, BEND_AT:EDGE_ROWS, :] = pack_sides(columns, ec == 0)
        columns = [window_ref[f, at["rows"], at["own_side"]] for f in range(SUMS)]
        columns += [latent_ref[k, at["tile_rows"], at["tile_side"]] for k in range(3)]
        side = pack_sides(columns, ec == 0)
        send_ref[2 * er + 1 - ec, 0:24, :] = side
        send_ref[3 - 2 * er - ec, 0:8, :] = side[at["corner"], :]

    for_quarter(body)


def krylov_kernel(
    coupling_ref, window_ref, latent_ref, got_ref, basis_ref, moments_ref, full_ref
):
    def body(er, ec, at):
        full_ref[0:SUMS] = window_ref[...]
        full_ref[SUMS:FIELDS, at["rows"], at["cols"]] = latent_ref[:, at["tile_rows"], at["tile_cols"]]
        side, corner = got_ref[2 * er + 1 - ec, 0:24, :], got_ref[3 - 2 * er - ec, 0:8, :]
        parts = [corner, side] if er == 0 else [side, corner]
        sides = jnp.concatenate(parts, axis=0)
        over = 2 * (1 - er) + ec
        bend = got_ref[over, BEND_AT:EDGE_ROWS, :]
        for f in range(FIELDS):
            for t in range(2):
                rows = slice(BLOCK * t + ABOVE[f], BLOCK * t + ABOVE[f] + DEPTH[f])
                full_ref[f, at["outer_rows"][f], 128 + 128 * t : 256 + 128 * t] = got_ref[over, rows, :]
            full_ref[f, at["outer_tile"], at["inner_cols"]] = unpack_side(bend, f, ec == 0)
            full_ref[f, :, at["outer_cols"]] = unpack_side(sides, f, ec == 1)

    for_quarter(body)
    mine = swapped(lax.axis_index("ens"))
    lon = place_of_lon()
    n_lon = lax.axis_size(LON[0]) * lax.axis_size(LON[1])
    shape = (ROWS, COLS)
    row = lax.broadcasted_iota(jnp.int32, shape, 0) + (
        lax.axis_index("lat") * ROWS + 16 * (mine // 2) - 8
    )
    col = lax.broadcasted_iota(jnp.int32, shape, 1) + (lon * COLS + 256 * (mine % 2) - 128)
    inside = (row >= 0) & (row < lax.axis_size("lat") * ROWS) & (col >= 0) & (col < n_lon * COLS)

    coupling = [
        [jnp.broadcast_to(coupling_ref[k : k + 1, j : j + 1], shape) for j in range(3)] for k in range(3)
    ]

    def mixed(field):
        laplace = []
        for x in field:
            beside = pltpu.roll(x, 1, 0) + pltpu.roll(x, ROWS - 1, 0)
            beside = beside + (pltpu.roll(x, 1, 1) + pltpu.roll(x, COLS - 1, 1))
            laplace.append(4.0 * x - beside)
        return [
            coupling[k][0] * laplace[0] + coupling[k][1] * laplace[1] + coupling[k][2] * laplace[2]
            for k in range(3)
        ]

    def operate(field):
        q = mixed(field)
        h = [full_ref[3 + k] for k in range(6)]
        x, y, z = field
        own = (h[0] * x + h[1] * y + h[2] * z, h[1] * x + h[3] * y + h[4] * z, h[2] * x + h[4] * y + h[5] * z)
        return [jnp.where(inside, SCALE * (a + b), 0.0) for a, b in zip(q, own)]

    prior = mixed([jnp.where(inside, full_ref[SUMS + k], 0.0) for k in range(3)])
    basis = [[jnp.where(inside, full_ref[k] - prior[k], 0.0) for k in range(3)]]
    for _ in range(ITERS):
        basis.append(operate(basis[-1]))
    own = [[x[8:24, 128:384] for x in field] for field in basis]
    for p in range(ITERS):
        for k in range(3):
            basis_ref[3 * p + k] = own[p][k]
    lane = lax.broadcasted_iota(jnp.int32, (1, 128), 1)
    moments = jnp.zeros((1, 128), jnp.float32)
    for k in range(2 * ITERS):
        a, b = own[k // 2], own[k - k // 2]
        product = a[0] * b[0] + a[1] * b[1] + a[2] * b[2]
        total = jnp.sum(jnp.sum(product, axis=0, keepdims=True), axis=1, keepdims=True)
        moments = jnp.where(lane == k, total, moments)
    moments_ref[...] = jnp.broadcast_to(moments[None], moments_ref.shape)


def krylov_weights(m):
    def inner(p, q, shift):
        terms = [p[i] * q[j] * m[i + j + shift] for i in range(len(p)) for j in range(len(q))]
        return sum(terms[1:], terms[0])

    def combine(p, factor, q):
        both = [x + factor * y for x, y in zip(p, q)]
        return both + p[len(q) :] + [factor * y for y in q[len(p) :]]

    one = jnp.ones_like(m[0])
    zero = jnp.zeros_like(m[0])
    weights, residual, direction = [], [one], [one]
    norm_now = m[0]
    for iteration in range(ITERS):
        step_size = norm_now / inner(direction, direction, 1)
        weights = combine(weights, step_size, direction)
        if iteration + 1 < ITERS:
            residual = combine(residual, -step_size, [zero] + direction)
            norm_next = inner(residual, residual, 0)
            direction = combine(residual, norm_next / norm_now, direction)
            norm_now = norm_next
    return [SCALE * w for w in weights]


def update_kernel(moments_ref, latent_ref, *refs):
    basis_refs, solution_ref = refs[:-1], refs[-1]
    moments = jnp.sum(moments_ref[...], axis=0)
    moments = [jnp.broadcast_to(moments[:, k : k + 1], (8, 128)) for k in range(2 * ITERS)]
    weights = [jnp.tile(w, (2, 2)) for w in krylov_weights(moments)]
    mine = lax.axis_index("ens")
    for back, basis_ref in zip((0, 1, 3, 2), basis_refs):
        q = swapped(lax.rem(mine + (4 - back), 4))
        rows = pl.ds(pl.multiple_of(16 * (q // 2), 8), 16)
        cols = pl.ds(pl.multiple_of(256 * (q % 2), 128), 256)
        for k in range(3):
            step = weights[0] * basis_ref[k] + weights[1] * basis_ref[3 + k] + weights[2] * basis_ref[6 + k]
            solution_ref[k, rows, cols] = latent_ref[k, rows, cols] + step


def f32(*shape):
    if INTERPRET:
        return jax.ShapeDtypeStruct(shape, jnp.float32)
    return pltpu.VMEM(shape, jnp.float32)


def near(*arrays):
    if INTERPRET:
        return arrays
    return tuple(pltpu.with_memory_space_constraint(a, pltpu.VMEM) for a in arrays)


def around_vertices():
    sizes = [lax.axis_size(axis) for axis in EVERY]
    n_lat, n_lon = sizes[1], sizes[2] * sizes[3]
    groups = {}
    for e, lat, lon in itertools.product(range(4), range(n_lat), range(n_lon)):
        lower, right = (e // 2 + lat) % 2, (e + lon) % 2
        vertex = (e, (lat + lower) % n_lat, (lon + right) % n_lon)
        groups.setdefault(vertex, {})[2 * lower + right] = (e * n_lat + lat) * n_lon + lon
    return [[group[q] for q in range(4)] for group in groups.values()]


def per_device(maxima, latent, coupling, local_precision):
    depth = maxima.shape[0]
    part = pl.pallas_call(
        gev_kernel,
        grid=(4,),
        in_specs=[
            pl.BlockSpec((depth, 8, COLS), lambda i: (0, i, 0)),
            pl.BlockSpec((3, 8, COLS), lambda i: (0, i, 0)),
        ],
        out_specs=VMEM,
        out_shape=f32(4, PART_ROWS, 128),
        interpret=INTERPRET,
        name="gev",
    )(maxima, latent)
    got = lax.all_to_all(part, "ens", 0, 0, tiled=True)
    window, halo = pl.pallas_call(
        join_kernel,
        in_specs=[VMEM] * 3,
        out_specs=[VMEM] * 2,
        out_shape=[f32(SUMS, ROWS, COLS), f32(4, EDGE_ROWS, 128)],
        interpret=INTERPRET,
        name="join",
    )(*near(got, latent, local_precision))
    halo = lax.all_to_all(halo, EVERY, 0, 0, axis_index_groups=around_vertices(), tiled=True)
    n_lat = lax.axis_size("lat")
    basis, moments = pl.pallas_call(
        krylov_kernel,
        in_specs=[VMEM] * 4,
        out_specs=[VMEM] * 2,
        out_shape=[f32(3 * ITERS, 16, 256), f32(n_lat, 1, 128)],
        scratch_shapes=[pltpu.VMEM((FIELDS, ROWS, COLS), jnp.float32)],
        interpret=INTERPRET,
        name="krylov",
    )(*near(coupling, window, latent, halo))

    def from_back(values, back):
        return lax.ppermute(values, "ens", [(e, (e + back) % 4) for e in range(4)])

    moments = lax.all_to_all(moments, "lat", 0, 0, tiled=True)
    moments = moments.sum(axis=0)
    others = []
    for back in (1, 3, 2):
        others.append(from_back(basis, back))
    rest = ("ens", *LON)
    moments = jnp.broadcast_to(moments, (lax.axis_size(rest), *moments.shape))
    moments = lax.all_to_all(moments, rest, 0, 0, tiled=True)
    return pl.pallas_call(
        update_kernel,
        in_specs=[VMEM] * 6,
        out_specs=VMEM,
        out_shape=jax.ShapeDtypeStruct((3, ROWS, COLS), jnp.float32),
        interpret=INTERPRET,
        name="update",
    )(*near(moments, latent, basis, *others))


def solution(mesh):
    split = Mesh(
        mesh.devices.reshape(mesh.shape["ens"], mesh.shape["lat"], -1, 2),
        ("ens", "lat", "lon_0", "lon_1"),
    )
    placed = (P("ens", "lat", LON), P(None, "lat", LON), P(), P(None, "lat", LON))
    return jax.shard_map(
        per_device, mesh=split, in_specs=placed, out_specs=P(None, "lat", LON), check_vma=False
    )
```

```python
import itertools

import jax
import jax.numpy as jnp
from jax import lax
from jax.experimental import pallas as pl
from jax.experimental.pallas import tpu as pltpu
from jax.sharding import Mesh
from jax.sharding import PartitionSpec as P


ITERS = 3
LON = ("lon_0", "lon_1")
EVERY = ("ens", "lat", *LON)
SCALE = 2.0**-10
LN2 = 0.6931471805599453
INTERPRET = False

ROWS, COLS = 32, 512
SUMS = 9
FIELDS = 12
HALO = 4
DEPTH = (3,) * 3 + (2,) * 6 + (4,) * 3
ABOVE = [sum(DEPTH[:f]) for f in range(FIELDS)]
EDGE_AT = SUMS * 2 * 16
SIDE_AT = EDGE_AT + 48
PART_ROWS = SIDE_AT + 24
BLOCK = 40
BEND_AT = 2 * BLOCK
EDGE_ROWS = BEND_AT + 8

VMEM = pl.BlockSpec(memory_space=pltpu.VMEM)


def lanes_of(field, shape):
    lane = lax.broadcasted_iota(jnp.int32, shape, 1)
    return (lane >= HALO * field) & (lane < HALO * (field + 1))


def pack_sides(columns, first):
    packed = jnp.zeros(columns[0].shape, jnp.float32)
    for f, x in enumerate(columns):
        shift = (HALO * f if first else HALO * f + HALO - 128) % 128
        packed = jnp.where(lanes_of(f, x.shape), pltpu.roll(x, shift, 1) if shift else x, packed)
    return packed


def unpack_side(packed, field, first):
    shift = (-HALO * field if first else 128 - HALO - HALO * field) % 128
    return pltpu.roll(packed, shift, 1) if shift else packed


def place_of_lon():
    return lax.axis_index(LON[0]) * lax.axis_size(LON[1]) + lax.axis_index(LON[1])


def swapped(e):
    return 2 * ((e // 2 + lax.axis_index("lat")) % 2) + (e + place_of_lon()) % 2


def gev_kernel(maxima_ref, latent_ref, part_ref):
    block = pl.program_id(0)
    for half in range(2):
        cols = slice(256 * half, 256 * half + 256)
        loc_par = 10.0 * latent_ref[0, :, cols]
        per_scale = jnp.exp(-latent_ref[1, :, cols])
        shape_par = 0.1 * latent_ref[2, :, cols]
        per_shape = -1.0 / (LN2 * shape_par)

        def add_one(m, sums):
            scaled = (maxima_ref[m, :, cols] - loc_par) * per_scale
            inside = 1.0 + shape_par * scaled
            power = jnp.log(inside) * per_shape
            rest = 1.0 - jnp.exp2(power)
            a = (shape_par + rest) / inside
            sa = scaled * a
            b = sa - 1.0
            c = power * rest * -LN2 - sa
            terms = (a, b, c, a * a, a * b, a * c, b * b, b * c, c * c)
            return tuple(s + t for s, t in zip(sums, terms))

        zero = jnp.zeros((8, 256), jnp.float32)
        sums = lax.fori_loop(0, maxima_ref.shape[0], add_one, (zero,) * SUMS, unroll=8)
        ka, kc = 10.0 * per_scale, 0.1 / shape_par
        factors = (ka, None, kc, ka * ka, ka, ka * kc, None, kc, kc * kc)
        sums = [s if k is None else s * k for s, k in zip(sums, factors)]

        owner = swapped(2 * (block // 2) + half)
        for f in range(SUMS):
            for t in range(2):
                at = pl.multiple_of((2 * f + t) * 16 + 8 * (block % 2), 8)
                part_ref[owner, pl.ds(at, 8), :] = sums[f][:, 128 * t : 128 * t + 128]

        def put_edge(to, top):
            for f in range(SUMS):
                rows = slice(0, DEPTH[f]) if top else slice(8 - DEPTH[f], 8)
                for t in range(2):
                    at = EDGE_AT + 24 * t + ABOVE[f]
                    part_ref[swapped(to), at : at + DEPTH[f], :] = sums[f][rows, 128 * t : 128 * t + 128]

        pl.when(block == 2)(lambda: put_edge(half, True))
        pl.when(block == 1)(lambda: put_edge(2 + half, False))

        near = slice(0, 128) if half else slice(128, 256)
        side = pack_sides([s[:, near] for s in sums], bool(half))

        def put_side(to, tile):
            part_ref[swapped(to), pl.ds(pl.multiple_of(SIDE_AT + 8 * tile, 8), 8), :] = side

        pl.when(block <= 2)(lambda: put_side(1 - half, block))
        pl.when(block >= 1)(lambda: put_side(3 - half, block - 1))


def placing(er, ec):
    return dict(
        rows=slice(8, 32) if er == 0 else slice(0, 24),
        cols=slice(128, 512) if ec == 0 else slice(0, 384),
        tile_rows=slice(0, 24) if er == 0 else slice(8, 32),
        tile_cols=slice(0, 384) if ec == 0 else slice(128, 512),
        inner_rows=[slice(24, 24 + d) if er == 0 else slice(8 - d, 8) for d in DEPTH],
        outer_rows=[slice(8 - d, 8) if er == 0 else slice(24, 24 + d) for d in DEPTH],
        outer_tile=slice(0, 8) if er == 0 else slice(24, 32),
        own_edge=[slice(8, 8 + d) if er == 0 else slice(24 - d, 24) for d in DEPTH],
        own_tile=slice(8, 16) if er == 0 else slice(16, 24),
        tile_edge=slice(0, HALO) if er == 0 else slice(32 - HALO, 32),
        tile_tile=slice(0, 8) if er == 0 else slice(24, 32),
        tile_inner=slice(256, 384) if ec == 0 else slice(128, 256),
        inner_cols=slice(384, 512) if ec == 0 else slice(0, 128),
        outer_cols=slice(0, 128) if ec == 0 else slice(384, 512),
        own_side=slice(128, 256) if ec == 0 else slice(256, 384),
        tile_side=slice(0, 128) if ec == 0 else slice(384, 512),
        corner=slice(0, 8) if er == 0 else slice(16, 24),
    )


def for_quarter(body):
    mine = swapped(lax.axis_index("ens"))
    for q in range(4):
        pl.when(mine == q)(lambda q=q: body(q // 2, q % 2, placing(q // 2, q % 2)))


def join_kernel(got_ref, latent_ref, precision_ref, window_ref, send_ref):
    def body(er, ec, at):
        def total(start, rows):
            cut = slice(start, start + rows)
            return got_ref[0, cut, :] + got_ref[1, cut, :] + got_ref[2, cut, :] + got_ref[3, cut, :]

        window_ref[...] = jnp.zeros(window_ref.shape, jnp.float32)
        sides = total(SIDE_AT, 24)
        for f in range(SUMS):
            window_ref[f, at["rows"], at["inner_cols"]] = unpack_side(sides, f, ec == 0)
            for t in range(2):
                cols = slice(128 + 128 * t, 256 + 128 * t)
                window_ref[f, 8:24, cols] = total((2 * f + t) * 16, 16)
                window_ref[f, at["inner_rows"][f], cols] = total(EDGE_AT + 24 * t + ABOVE[f], DEPTH[f])
        for k, diagonal in enumerate((3, 6, 8)):
            level = precision_ref[k, at["tile_rows"], at["tile_cols"]]
            here = latent_ref[k, at["tile_rows"], at["tile_cols"]]
            there = (at["rows"], at["cols"])
            window_ref[k, *there] = window_ref[k, *there] - level * here
            window_ref[diagonal, *there] = window_ref[diagonal, *there] + level
        over = 2 * (1 - er) + ec
        for f in range(FIELDS):
            for t in range(2):
                rows = slice(BLOCK * t + ABOVE[f], BLOCK * t + ABOVE[f] + DEPTH[f])
                tile_cols = slice(256 * ec + 128 * t, 256 * ec + 128 * t + 128)
                send_ref[over, rows, :] = (
                    window_ref[f, at["own_edge"][f], 128 + 128 * t : 256 + 128 * t]
                    if f < SUMS
                    else latent_ref[f - SUMS, at["tile_edge"], tile_cols]
                )
        columns = [window_ref[f, at["own_tile"], at["inner_cols"]] for f in range(SUMS)]
        columns += [latent_ref[k, at["tile_tile"], at["tile_inner"]] for k in range(3)]
        send_ref[over, BEND_AT:EDGE_ROWS, :] = pack_sides(columns, ec == 0)
        columns = [window_ref[f, at["rows"], at["own_side"]] for f in range(SUMS)]
        columns += [latent_ref[k, at["tile_rows"], at["tile_side"]] for k in range(3)]
        side = pack_sides(columns, ec == 0)
        send_ref[2 * er + 1 - ec, 0:24, :] = side
        send_ref[3 - 2 * er - ec, 0:8, :] = side[at["corner"], :]

    for_quarter(body)


def krylov_kernel(
    coupling_ref, window_ref, latent_ref, got_ref, basis_ref, moments_ref, full_ref
):
    def body(er, ec, at):
        full_ref[0:SUMS] = window_ref[...]
        full_ref[SUMS:FIELDS, at["rows"], at["cols"]] = latent_ref[:, at["tile_rows"], at["tile_cols"]]
        side, corner = got_ref[2 * er + 1 - ec, 0:24, :], got_ref[3 - 2 * er - ec, 0:8, :]
        parts = [corner, side] if er == 0 else [side, corner]
        sides = jnp.concatenate(parts, axis=0)
        over = 2 * (1 - er) + ec
        bend = got_ref[over, BEND_AT:EDGE_ROWS, :]
        for f in range(FIELDS):
            for t in range(2):
                rows = slice(BLOCK * t + ABOVE[f], BLOCK * t + ABOVE[f] + DEPTH[f])
                full_ref[f, at["outer_rows"][f], 128 + 128 * t : 256 + 128 * t] = got_ref[over, rows, :]
            full_ref[f, at["outer_tile"], at["inner_cols"]] = unpack_side(bend, f, ec == 0)
            full_ref[f, :, at["outer_cols"]] = unpack_side(sides, f, ec == 1)

    for_quarter(body)
    mine = swapped(lax.axis_index("ens"))
    lon = place_of_lon()
    n_lon = lax.axis_size(LON[0]) * lax.axis_size(LON[1])
    shape = (ROWS, COLS)
    row = lax.broadcasted_iota(jnp.int32, shape, 0) + (
        lax.axis_index("lat") * ROWS + 16 * (mine // 2) - 8
    )
    col = lax.broadcasted_iota(jnp.int32, shape, 1) + (lon * COLS + 256 * (mine % 2) - 128)
    inside = (row >= 0) & (row < lax.axis_size("lat") * ROWS) & (col >= 0) & (col < n_lon * COLS)

    coupling = [
        [jnp.broadcast_to(coupling_ref[k : k + 1, j : j + 1], shape) for j in range(3)] for k in range(3)
    ]

    def mixed(field):
        laplace = []
        for x in field:
            beside = pltpu.roll(x, 1, 0) + pltpu.roll(x, ROWS - 1, 0)
            beside = beside + (pltpu.roll(x, 1, 1) + pltpu.roll(x, COLS - 1, 1))
            laplace.append(4.0 * x - beside)
        return [
            coupling[k][0] * laplace[0] + coupling[k][1] * laplace[1] + coupling[k][2] * laplace[2]
            for k in range(3)
        ]

    def operate(field):
        q = mixed(field)
        h = [full_ref[3 + k] for k in range(6)]
        x, y, z = field
        own = (h[0] * x + h[1] * y + h[2] * z, h[1] * x + h[3] * y + h[4] * z, h[2] * x + h[4] * y + h[5] * z)
        return [jnp.where(inside, SCALE * (a + b), 0.0) for a, b in zip(q, own)]

    prior = mixed([jnp.where(inside, full_ref[SUMS + k], 0.0) for k in range(3)])
    basis = [[jnp.where(inside, full_ref[k] - prior[k], 0.0) for k in range(3)]]
    for _ in range(ITERS):
        basis.append(operate(basis[-1]))
    own = [[x[8:24, 128:384] for x in field] for field in basis]
    for p in range(ITERS):
        for k in range(3):
            basis_ref[3 * p + k] = own[p][k]
    lane = lax.broadcasted_iota(jnp.int32, (1, 128), 1)
    moments = jnp.zeros((1, 128), jnp.float32)
    for k in range(2 * ITERS):
        a, b = own[k // 2], own[k - k // 2]
        product = a[0] * b[0] + a[1] * b[1] + a[2] * b[2]
        total = jnp.sum(jnp.sum(product, axis=0, keepdims=True), axis=1, keepdims=True)
        moments = jnp.where(lane == k, total, moments)
    moments_ref[...] = jnp.broadcast_to(moments[None], moments_ref.shape)


def krylov_weights(m):
    def inner(p, q, shift):
        terms = [p[i] * q[j] * m[i + j + shift] for i in range(len(p)) for j in range(len(q))]
        return sum(terms[1:], terms[0])

    def combine(p, factor, q):
        both = [x + factor * y for x, y in zip(p, q)]
        return both + p[len(q) :] + [factor * y for y in q[len(p) :]]

    one = jnp.ones_like(m[0])
    zero = jnp.zeros_like(m[0])
    weights, residual, direction = [], [one], [one]
    norm_now = m[0]
    for iteration in range(ITERS):
        step_size = norm_now / inner(direction, direction, 1)
        weights = combine(weights, step_size, direction)
        if iteration + 1 < ITERS:
            residual = combine(residual, -step_size, [zero] + direction)
            norm_next = inner(residual, residual, 0)
            direction = combine(residual, norm_next / norm_now, direction)
            norm_now = norm_next
    return [SCALE * w for w in weights]


def update_kernel(moments_ref, latent_ref, *refs):
    basis_refs, solution_ref = refs[:-1], refs[-1]
    moments = jnp.sum(moments_ref[...], axis=0)
    moments = [jnp.broadcast_to(moments[:, k : k + 1], (8, 128)) for k in range(2 * ITERS)]
    weights = [jnp.tile(w, (2, 2)) for w in krylov_weights(moments)]
    mine = lax.axis_index("ens")
    for back, basis_ref in zip((0, 1, 3, 2), basis_refs):
        q = swapped(lax.rem(mine + (4 - back), 4))
        rows = pl.ds(pl.multiple_of(16 * (q // 2), 8), 16)
        cols = pl.ds(pl.multiple_of(256 * (q % 2), 128), 256)
        for k in range(3):
            step = weights[0] * basis_ref[k] + weights[1] * basis_ref[3 + k] + weights[2] * basis_ref[6 + k]
            solution_ref[k, rows, cols] = latent_ref[k, rows, cols] + step


def f32(*shape):
    if INTERPRET:
        return jax.ShapeDtypeStruct(shape, jnp.float32)
    return pltpu.VMEM(shape, jnp.float32)


def near(*arrays):
    if INTERPRET:
        return arrays
    return tuple(pltpu.with_memory_space_constraint(a, pltpu.VMEM) for a in arrays)


def around_vertices():
    sizes = [lax.axis_size(axis) for axis in EVERY]
    n_lat, n_lon = sizes[1], sizes[2] * sizes[3]
    groups = {}
    for e, lat, lon in itertools.product(range(4), range(n_lat), range(n_lon)):
        lower, right = (e // 2 + lat) % 2, (e + lon) % 2
        vertex = (e, (lat + lower) % n_lat, (lon + right) % n_lon)
        groups.setdefault(vertex, {})[2 * lower + right] = (e * n_lat + lat) * n_lon + lon
    return [[group[q] for q in range(4)] for group in groups.values()]


def per_device(maxima, latent, coupling, local_precision):
    depth = maxima.shape[0]
    part = pl.pallas_call(
        gev_kernel,
        grid=(4,),
        in_specs=[
            pl.BlockSpec((depth, 8, COLS), lambda i: (0, i, 0)),
            pl.BlockSpec((3, 8, COLS), lambda i: (0, i, 0)),
        ],
        out_specs=VMEM,
        out_shape=f32(4, PART_ROWS, 128),
        interpret=INTERPRET,
        name="gev",
    )(maxima, latent)
    got = lax.all_to_all(part, "ens", 0, 0, tiled=True)
    window, halo = pl.pallas_call(
        join_kernel,
        in_specs=[VMEM] * 3,
        out_specs=[VMEM] * 2,
        out_shape=[f32(SUMS, ROWS, COLS), f32(4, EDGE_ROWS, 128)],
        interpret=INTERPRET,
        name="join",
    )(*near(got, latent, local_precision))
    halo = lax.all_to_all(halo, EVERY, 0, 0, axis_index_groups=around_vertices(), tiled=True)
    n_column = lax.axis_size(("lat", LON[1]))
    basis, moments = pl.pallas_call(
        krylov_kernel,
        in_specs=[VMEM] * 4,
        out_specs=[VMEM] * 2,
        out_shape=[f32(3 * ITERS, 16, 256), f32(n_column, 1, 128)],
        scratch_shapes=[pltpu.VMEM((FIELDS, ROWS, COLS), jnp.float32)],
        interpret=INTERPRET,
        name="krylov",
    )(*near(coupling, window, latent, halo))

    def from_back(values, back):
        return lax.ppermute(values, "ens", [(e, (e + back) % 4) for e in range(4)])

    moments = lax.all_to_all(moments, ("lat", LON[1]), 0, 0, tiled=True)
    moments = moments.sum(axis=0)
    others = []
    for back in (1, 3, 2):
        others.append(from_back(basis, back))
    rest = ("ens", LON[0])
    moments = jnp.broadcast_to(moments, (lax.axis_size(rest), *moments.shape))
    moments = lax.all_to_all(moments, rest, 0, 0, tiled=True)
    return pl.pallas_call(
        update_kernel,
        in_specs=[VMEM] * 6,
        out_specs=VMEM,
        out_shape=jax.ShapeDtypeStruct((3, ROWS, COLS), jnp.float32),
        interpret=INTERPRET,
        name="update",
    )(*near(moments, latent, basis, *others))


def solution(mesh):
    split = Mesh(
        mesh.devices.reshape(mesh.shape["ens"], mesh.shape["lat"], -1, 2),
        ("ens", "lat", "lon_0", "lon_1"),
    )
    placed = (P("ens", "lat", LON), P(None, "lat", LON), P(), P(None, "lat", LON))
    return jax.shard_map(
        per_device, mesh=split, in_specs=placed, out_specs=P(None, "lat", LON), check_vma=False
    )
```

```python
import itertools

import jax
import jax.numpy as jnp
from jax import lax
from jax.experimental import pallas as pl
from jax.experimental.pallas import tpu as pltpu
from jax.sharding import Mesh
from jax.sharding import PartitionSpec as P


ITERS = 3
LON = ("lon_0", "lon_1")
EVERY = ("ens", "lat", *LON)
SCALE = 2.0**-10
LN2 = 0.6931471805599453
INTERPRET = False

ROWS, COLS = 32, 512
SUMS = 9
FIELDS = 12
HALO = 4
DEPTH = (3,) * 3 + (2,) * 6 + (4,) * 3
ABOVE = [sum(DEPTH[:f]) for f in range(FIELDS)]
SIDE_AT = SUMS * 2 * 16
EDGE_AT = SIDE_AT + 8
PART_ROWS = EDGE_AT + 48
BLOCK = 33
BEND_AT = 72
EDGE_ROWS = BEND_AT + 8

VMEM = pl.BlockSpec(memory_space=pltpu.VMEM)


def lanes_of(field, shape):
    lane = lax.broadcasted_iota(jnp.int32, shape, 1)
    return (lane >= HALO * field) & (lane < HALO * (field + 1))


def pack_sides(columns, first):
    packed = jnp.zeros(columns[0].shape, jnp.float32)
    for f, x in enumerate(columns):
        shift = (HALO * f if first else HALO * f + HALO - 128) % 128
        packed = jnp.where(lanes_of(f, x.shape), pltpu.roll(x, shift, 1) if shift else x, packed)
    return packed


def unpack_side(packed, field, first):
    shift = (-HALO * field if first else 128 - HALO - HALO * field) % 128
    return pltpu.roll(packed, shift, 1) if shift else packed


def place_of_lon():
    return lax.axis_index(LON[0]) * lax.axis_size(LON[1]) + lax.axis_index(LON[1])


def swapped(e):
    return 2 * ((e // 2 + lax.axis_index("lat")) % 2) + (e + place_of_lon()) % 2


def gev_kernel(maxima_ref, latent_ref, part_ref):
    block = pl.program_id(0)
    for half in range(2):
        cols = slice(256 * half, 256 * half + 256)
        loc_par = 10.0 * latent_ref[0, :, cols]
        per_scale = jnp.exp(-latent_ref[1, :, cols])
        shape_par = 0.1 * latent_ref[2, :, cols]
        per_shape = -1.0 / (LN2 * shape_par)

        def add_one(m, sums):
            scaled = (maxima_ref[m, :, cols] - loc_par) * per_scale
            inside = 1.0 + shape_par * scaled
            power = jnp.log(inside) * per_shape
            rest = 1.0 - jnp.exp2(power)
            a = (shape_par + rest) / inside
            sa = scaled * a
            b = sa - 1.0
            c = power * rest * -LN2 - sa
            terms = (a, b, c, a * a, a * b, a * c, b * b, b * c, c * c)
            return tuple(s + t for s, t in zip(sums, terms))

        zero = jnp.zeros((8, 256), jnp.float32)
        sums = lax.fori_loop(0, maxima_ref.shape[0], add_one, (zero,) * SUMS, unroll=16)
        ka, kc = 10.0 * per_scale, 0.1 / shape_par
        factors = (ka, None, kc, ka * ka, ka, ka * kc, None, kc, kc * kc)
        sums = [s if k is None else s * k for s, k in zip(sums, factors)]

        owner = swapped(2 * (block // 2) + half)
        for f in range(SUMS):
            for t in range(2):
                at = pl.multiple_of((2 * f + t) * 16 + 8 * (block % 2), 8)
                part_ref[owner, pl.ds(at, 8), :] = sums[f][:, 128 * t : 128 * t + 128]

        def put_edge(to, top):
            for f in range(SUMS):
                rows = slice(0, DEPTH[f]) if top else slice(8 - DEPTH[f], 8)
                for t in range(2):
                    at = EDGE_AT + 21 * t + ABOVE[f]
                    part_ref[swapped(to), at : at + DEPTH[f], :] = sums[f][rows, 128 * t : 128 * t + 128]

        pl.when(block == 2)(lambda: put_edge(half, True))
        pl.when(block == 1)(lambda: put_edge(2 + half, False))

        near = slice(0, 128) if half else slice(128, 256)
        side = pack_sides([s[:, near] for s in sums], bool(half))

        def put_side(to, tile):
            at = HALO * SUMS * tile
            shifted = pltpu.roll(side, at, 1) if at else side
            here = part_ref[swapped(to), SIDE_AT : SIDE_AT + 8, :]
            lane = lax.broadcasted_iota(jnp.int32, (8, 128), 1)
            part_ref[swapped(to), SIDE_AT : SIDE_AT + 8, :] = jnp.where(lane >= at, shifted, here)

        for i in range(3):
            pl.when(block == i)(lambda i=i: put_side(1 - half, i))
            pl.when(block == i + 1)(lambda i=i: put_side(3 - half, i))


def placing(er, ec):
    return dict(
        rows=slice(8, 32) if er == 0 else slice(0, 24),
        cols=slice(128, 512) if ec == 0 else slice(0, 384),
        tile_rows=slice(0, 24) if er == 0 else slice(8, 32),
        tile_cols=slice(0, 384) if ec == 0 else slice(128, 512),
        inner_rows=[slice(24, 24 + d) if er == 0 else slice(8 - d, 8) for d in DEPTH],
        outer_rows=[slice(8 - d, 8) if er == 0 else slice(24, 24 + d) for d in DEPTH],
        outer_tile=slice(0, 8) if er == 0 else slice(24, 32),
        own_edge=[slice(8, 8 + d) if er == 0 else slice(24 - d, 24) for d in DEPTH],
        own_tile=slice(8, 16) if er == 0 else slice(16, 24),
        tile_edge=slice(0, HALO) if er == 0 else slice(32 - HALO, 32),
        tile_tile=slice(0, 8) if er == 0 else slice(24, 32),
        tile_inner=slice(256, 384) if ec == 0 else slice(128, 256),
        inner_cols=slice(384, 512) if ec == 0 else slice(0, 128),
        outer_cols=slice(0, 128) if ec == 0 else slice(384, 512),
        own_side=slice(128, 256) if ec == 0 else slice(256, 384),
        tile_side=slice(0, 128) if ec == 0 else slice(384, 512),
        corner=slice(0, 8) if er == 0 else slice(16, 24),
    )


def for_quarter(body):
    mine = swapped(lax.axis_index("ens"))
    for q in range(4):
        pl.when(mine == q)(lambda q=q: body(q // 2, q % 2, placing(q // 2, q % 2)))


def join_kernel(got_ref, latent_ref, precision_ref, window_ref, send_ref):
    def body(er, ec, at):
        def total(start, rows):
            cut = slice(start, start + rows)
            return got_ref[0, cut, :] + got_ref[1, cut, :] + got_ref[2, cut, :] + got_ref[3, cut, :]

        window_ref[...] = jnp.zeros(window_ref.shape, jnp.float32)
        sides = total(SIDE_AT, 8)
        sides = [pltpu.roll(sides, 128 - HALO * SUMS * i, 1) if i else sides for i in range(3)]
        sides = jnp.concatenate(sides, axis=0)
        for f in range(SUMS):
            window_ref[f, at["rows"], at["inner_cols"]] = unpack_side(sides, f, ec == 0)
            for t in range(2):
                cols = slice(128 + 128 * t, 256 + 128 * t)
                window_ref[f, 8:24, cols] = total((2 * f + t) * 16, 16)
                window_ref[f, at["inner_rows"][f], cols] = total(EDGE_AT + 21 * t + ABOVE[f], DEPTH[f])
        for k, diagonal in enumerate((3, 6, 8)):
            level = precision_ref[k, at["tile_rows"], at["tile_cols"]]
            here = latent_ref[k, at["tile_rows"], at["tile_cols"]]
            there = (at["rows"], at["cols"])
            window_ref[k, *there] = window_ref[k, *there] - level * here
            window_ref[diagonal, *there] = window_ref[diagonal, *there] + level
        over = 2 * (1 - er) + ec
        for f in range(FIELDS):
            for t in range(2):
                rows = slice(BLOCK * t + ABOVE[f], BLOCK * t + ABOVE[f] + DEPTH[f])
                tile_cols = slice(256 * ec + 128 * t, 256 * ec + 128 * t + 128)
                send_ref[over, rows, :] = (
                    window_ref[f, at["own_edge"][f], 128 + 128 * t : 256 + 128 * t]
                    if f < SUMS
                    else latent_ref[f - SUMS, at["tile_edge"], tile_cols]
                )
        columns = [window_ref[f, at["own_tile"], at["inner_cols"]] for f in range(SUMS)]
        columns += [latent_ref[k, at["tile_tile"], at["tile_inner"]] for k in range(3)]
        send_ref[over, BEND_AT:EDGE_ROWS, :] = pack_sides(columns, ec == 0)
        columns = [window_ref[f, at["rows"], at["own_side"]] for f in range(SUMS)]
        columns += [latent_ref[k, at["tile_rows"], at["tile_side"]] for k in range(3)]
        side = pack_sides(columns, ec == 0)
        send_ref[2 * er + 1 - ec, 0:24, :] = side
        send_ref[3 - 2 * er - ec, 0:8, :] = side[at["corner"], :]

    for_quarter(body)


def krylov_kernel(
    coupling_ref, window_ref, latent_ref, got_ref, basis_ref, moments_ref, full_ref
):
    def body(er, ec, at):
        full_ref[0:SUMS] = window_ref[...]
        full_ref[SUMS:FIELDS, at["rows"], at["cols"]] = latent_ref[:, at["tile_rows"], at["tile_cols"]]
        side, corner = got_ref[2 * er + 1 - ec, 0:24, :], got_ref[3 - 2 * er - ec, 0:8, :]
        parts = [corner, side] if er == 0 else [side, corner]
        sides = jnp.concatenate(parts, axis=0)
        over = 2 * (1 - er) + ec
        bend = got_ref[over, BEND_AT:EDGE_ROWS, :]
        for f in range(FIELDS):
            for t in range(2):
                rows = slice(BLOCK * t + ABOVE[f], BLOCK * t + ABOVE[f] + DEPTH[f])
                full_ref[f, at["outer_rows"][f], 128 + 128 * t : 256 + 128 * t] = got_ref[over, rows, :]
            full_ref[f, at["outer_tile"], at["inner_cols"]] = unpack_side(bend, f, ec == 0)
            full_ref[f, :, at["outer_cols"]] = unpack_side(sides, f, ec == 1)

    for_quarter(body)
    mine = swapped(lax.axis_index("ens"))
    lon = place_of_lon()
    n_lon = lax.axis_size(LON[0]) * lax.axis_size(LON[1])
    shape = (ROWS, COLS)
    row = lax.broadcasted_iota(jnp.int32, shape, 0) + (
        lax.axis_index("lat") * ROWS + 16 * (mine // 2) - 8
    )
    col = lax.broadcasted_iota(jnp.int32, shape, 1) + (lon * COLS + 256 * (mine % 2) - 128)
    inside = (row >= 0) & (row < lax.axis_size("lat") * ROWS) & (col >= 0) & (col < n_lon * COLS)

    coupling = [
        [jnp.broadcast_to(coupling_ref[k : k + 1, j : j + 1], shape) for j in range(3)] for k in range(3)
    ]

    def mixed(field):
        laplace = []
        for x in field:
            beside = pltpu.roll(x, 1, 0) + pltpu.roll(x, ROWS - 1, 0)
            beside = beside + (pltpu.roll(x, 1, 1) + pltpu.roll(x, COLS - 1, 1))
            laplace.append(4.0 * x - beside)
        return [
            coupling[k][0] * laplace[0] + coupling[k][1] * laplace[1] + coupling[k][2] * laplace[2]
            for k in range(3)
        ]

    def operate(field):
        q = mixed(field)
        h = [full_ref[3 + k] for k in range(6)]
        x, y, z = field
        own = (h[0] * x + h[1] * y + h[2] * z, h[1] * x + h[3] * y + h[4] * z, h[2] * x + h[4] * y + h[5] * z)
        return [jnp.where(inside, SCALE * (a + b), 0.0) for a, b in zip(q, own)]

    prior = mixed([jnp.where(inside, full_ref[SUMS + k], 0.0) for k in range(3)])
    basis = [[jnp.where(inside, full_ref[k] - prior[k], 0.0) for k in range(3)]]
    for _ in range(ITERS):
        basis.append(operate(basis[-1]))
    own = [[x[8:24, 128:384] for x in field] for field in basis]
    for p in range(ITERS):
        for k in range(3):
            basis_ref[3 * p + k] = own[p][k]
    lane = lax.broadcasted_iota(jnp.int32, (1, 128), 1)
    moments = jnp.zeros((1, 128), jnp.float32)
    for k in range(2 * ITERS):
        a, b = own[k // 2], own[k - k // 2]
        product = a[0] * b[0] + a[1] * b[1] + a[2] * b[2]
        total = jnp.sum(jnp.sum(product, axis=0, keepdims=True), axis=1, keepdims=True)
        moments = jnp.where(lane == k, total, moments)
    moments_ref[...] = jnp.broadcast_to(moments[None], moments_ref.shape)


def krylov_weights(m):
    def inner(p, q, shift):
        terms = [p[i] * q[j] * m[i + j + shift] for i in range(len(p)) for j in range(len(q))]
        return sum(terms[1:], terms[0])

    def combine(p, factor, q):
        both = [x + factor * y for x, y in zip(p, q)]
        return both + p[len(q) :] + [factor * y for y in q[len(p) :]]

    one = jnp.ones_like(m[0])
    zero = jnp.zeros_like(m[0])
    weights, residual, direction = [], [one], [one]
    norm_now = m[0]
    for iteration in range(ITERS):
        step_size = norm_now / inner(direction, direction, 1)
        weights = combine(weights, step_size, direction)
        if iteration + 1 < ITERS:
            residual = combine(residual, -step_size, [zero] + direction)
            norm_next = inner(residual, residual, 0)
            direction = combine(residual, norm_next / norm_now, direction)
            norm_now = norm_next
    return [SCALE * w for w in weights]


def update_kernel(moments_ref, latent_ref, *refs):
    basis_refs, solution_ref = refs[:-1], refs[-1]
    moments = jnp.sum(moments_ref[...], axis=0)
    moments = [jnp.broadcast_to(moments[:, k : k + 1], (8, 128)) for k in range(2 * ITERS)]
    weights = [jnp.tile(w, (2, 2)) for w in krylov_weights(moments)]
    mine = lax.axis_index("ens")
    for back, basis_ref in zip((0, 3, 1, 2), basis_refs):
        q = swapped(lax.rem(mine + (4 - back), 4))
        rows = pl.ds(pl.multiple_of(16 * (q // 2), 8), 16)
        cols = pl.ds(pl.multiple_of(256 * (q % 2), 128), 256)
        for k in range(3):
            step = weights[0] * basis_ref[k] + weights[1] * basis_ref[3 + k] + weights[2] * basis_ref[6 + k]
            solution_ref[k, rows, cols] = latent_ref[k, rows, cols] + step


def f32(*shape):
    if INTERPRET:
        return jax.ShapeDtypeStruct(shape, jnp.float32)
    return pltpu.VMEM(shape, jnp.float32)


def near(*arrays):
    if INTERPRET:
        return arrays
    return tuple(pltpu.with_memory_space_constraint(a, pltpu.VMEM) for a in arrays)


def around_vertices():
    sizes = [lax.axis_size(axis) for axis in EVERY]
    n_lat, n_lon = sizes[1], sizes[2] * sizes[3]
    groups = {}
    for e, lat, lon in itertools.product(range(4), range(n_lat), range(n_lon)):
        lower, right = (e // 2 + lat) % 2, (e + lon) % 2
        vertex = (e, (lat + lower) % n_lat, (lon + right) % n_lon)
        groups.setdefault(vertex, {})[2 * lower + right] = (e * n_lat + lat) * n_lon + lon
    return [[group[q] for q in range(4)] for group in groups.values()]


def per_device(maxima, latent, coupling, local_precision):
    depth = maxima.shape[0]
    part = pl.pallas_call(
        gev_kernel,
        grid=(4,),
        in_specs=[
            pl.BlockSpec((depth, 8, COLS), lambda i: (0, i, 0)),
            pl.BlockSpec((3, 8, COLS), lambda i: (0, i, 0)),
        ],
        out_specs=VMEM,
        out_shape=f32(4, PART_ROWS, 128),
        interpret=INTERPRET,
        name="gev",
    )(maxima, latent)
    got = lax.all_to_all(part, "ens", 0, 0, tiled=True)
    window, halo = pl.pallas_call(
        join_kernel,
        in_specs=[VMEM] * 3,
        out_specs=[VMEM] * 2,
        out_shape=[f32(SUMS, ROWS, COLS), f32(4, EDGE_ROWS, 128)],
        interpret=INTERPRET,
        name="join",
    )(*near(got, latent, local_precision))
    halo = lax.all_to_all(halo, EVERY, 0, 0, axis_index_groups=around_vertices(), tiled=True)
    n_column = lax.axis_size(("lat", LON[1]))
    basis, moments = pl.pallas_call(
        krylov_kernel,
        in_specs=[VMEM] * 4,
        out_specs=[VMEM] * 2,
        out_shape=[f32(3 * ITERS, 16, 256), f32(n_column, 1, 128)],
        scratch_shapes=[pltpu.VMEM((FIELDS, ROWS, COLS), jnp.float32)],
        interpret=INTERPRET,
        name="krylov",
    )(*near(coupling, window, latent, halo))

    def from_back(values, back):
        return lax.ppermute(values, "ens", [(e, (e + back) % 4) for e in range(4)])

    moments = lax.all_to_all(moments, ("lat", LON[1]), 0, 0, tiled=True)
    moments = moments.sum(axis=0)
    others = []
    for back in (3, 1, 2):
        others.append(from_back(basis, back))
    rest = ("ens", LON[0])
    moments = jnp.broadcast_to(moments, (lax.axis_size(rest), *moments.shape))
    moments = lax.all_to_all(moments, rest, 0, 0, tiled=True)
    return pl.pallas_call(
        update_kernel,
        in_specs=[VMEM] * 6,
        out_specs=VMEM,
        out_shape=jax.ShapeDtypeStruct((3, ROWS, COLS), jnp.float32),
        interpret=INTERPRET,
        name="update",
    )(*near(moments, latent, basis, *others))


def solution(mesh):
    split = Mesh(
        mesh.devices.reshape(mesh.shape["ens"], mesh.shape["lat"], -1, 2),
        ("ens", "lat", "lon_0", "lon_1"),
    )
    placed = (P("ens", "lat", LON), P(None, "lat", LON), P(), P(None, "lat", LON))
    return jax.shard_map(
        per_device, mesh=split, in_specs=placed, out_specs=P(None, "lat", LON), check_vma=False
    )
```
